512 devices in a mesh: tm: 64 (over y, z), chan: 8 (over x, core).
Axes of the slice: x: 4, y: 4, z: 16, core: 2. Of those that a mesh axis runs over, the one named last changes fastest.
Arguments:
- data: bfloat16 [6144, 8192], P('chan', 'tm'), may hold values from -6 to 6
- basis: float32 [6, 61], replicated, may hold values from -0.75 to 0.75
- templates: float32 [2048, 192], P(('tm', 'chan')), may hold values from -18 to 18
- spike_offset: int32 [2048], P('tm'), may hold values from 0 to 127, as said below
- spike_unit: int32 [2048], P('tm'), may hold values from 0 to 2047, as said below
- spike_amp: float32 [2048], P('tm'), may hold values from 0.5 to 2
- seg_count: int32 [64], P('tm'), may hold values from 16 to 32
- neighbors: int32 [2048, 32], replicated, may hold values from 0 to 6143, as said below
Outputs:
- residual: bfloat16 [6144, 8192], P('chan', 'tm')
- new_templates: float32 [2048, 192], P(('tm', 'chan'))
The draws below stay inside these ranges and needn't reach their ends.
Inputs may be any that keep to these rules, and one draw needn't show every extreme that they name: `spike_offset`: in every segment slot i < 8 has an offset below 30, slot i with 8 <= i < 16 an offset of 98 or more. `spike_unit`: in every segment slot i < 16 names a unit of the (i mod 8)-th of 8 equal bands of unit numbers. `neighbors`: row k holds 32 consecutive channels, rising, whose first differs by at most 16 from floor(k * 6112 / 2047).
All inputs are finite; a program needn't handle non-finite values.
Results may differ from the reference program's by a relative error of at most 0.0034.
Values may be sent and summed in bfloat16 or wider, within the bound.
A program may use at most 64 MiB of HBM per device.

```python
import math
import jax
import jax.numpy as jnp
from jax import lax

CHANNELS = 6144
UNITS = 2048
NBR = 32
NB = 6
HALF = 30
EDGE = 8
TS = 128
SLOTS = 32
NT = 61
COEF = 192
SEGMENTS = 64
SAMPLES = 8192
SPIKES = 2048


def draw_spike_offset(key, part):
    key_start, key_end, key_any = jax.random.split(key, 3)
    slot_index = jnp.arange(SLOTS, dtype=jnp.int32)[None, :]
    near_start = jax.random.randint(key_start, (SEGMENTS, SLOTS), 0, HALF, dtype=jnp.int32)
    near_end = jax.random.randint(key_end, (SEGMENTS, SLOTS), TS - HALF, TS, dtype=jnp.int32)
    anywhere = jax.random.randint(key_any, (SEGMENTS, SLOTS), 0, TS, dtype=jnp.int32)
    result = jnp.where(slot_index < EDGE, near_start, jnp.where(slot_index < 2 * EDGE, near_end, anywhere))
    result = result.at[0, 0].set(0).at[0, EDGE].set(TS - 1)
    return result.reshape(-1)


def draw_spike_unit(key, part):
    key_band, key_first, key_second, key_order = jax.random.split(key, 4)
    band = UNITS // EDGE
    slot_index = jnp.arange(SLOTS, dtype=jnp.int32)[None, :]
    edge_units = slot_index % EDGE * band + jax.random.randint(key_band, (SEGMENTS, SLOTS), 0, band, dtype=jnp.int32)
    first_pick = jax.random.randint(key_first, (SEGMENTS, SLOTS), 0, UNITS, dtype=jnp.int32)
    second_pick = jax.random.randint(key_second, (SEGMENTS, SLOTS), 0, UNITS, dtype=jnp.int32)
    ranked = first_pick * second_pick // UNITS
    order = jax.random.permutation(key_order, jnp.arange(UNITS, dtype=jnp.int32))
    busy_units = order[ranked]
    result = jnp.where(slot_index < 2 * EDGE, edge_units, busy_units)
    result = result.at[0, 0].set(0).at[0, EDGE - 1].set(UNITS - 1)
    return result.reshape(-1)


def draw_seg_count(key, part):
    key_count, key_where = jax.random.split(key)
    counts = jax.random.randint(key_count, (SEGMENTS,), 2 * EDGE, SLOTS + 1, dtype=jnp.int32)
    where_full = jax.random.randint(key_where, (), 0, SEGMENTS, dtype=jnp.int32)
    where_low = (where_full + 1) % SEGMENTS
    position = jnp.arange(SEGMENTS, dtype=jnp.int32)
    counts = jnp.where(position == where_low, 2 * EDGE, counts)
    counts = jnp.where(position == where_full, SLOTS, counts)
    return counts


def draw_neighbors(key, part):
    unit_index = jnp.arange(UNITS, dtype=jnp.int32)
    centre = unit_index * (CHANNELS - NBR) // (UNITS - 1)
    jitter = jax.random.randint(key, (UNITS,), -(NBR // 2), NBR // 2 + 1, dtype=jnp.int32)
    start = jnp.clip(centre + jitter, 0, CHANNELS - NBR)
    start = jnp.where(unit_index == 0, 0, jnp.where(unit_index == UNITS - 1, CHANNELS - NBR, start))
    return start[:, None] + jnp.arange(NBR, dtype=jnp.int32)[None, :]


def block_levels(key, extent, cuts, low, high):
    gain = 1.0
    for axis_at, blocks in cuts:
        steps = jax.random.uniform(jax.random.fold_in(jax.random.fold_in(key, 6), axis_at), (blocks,), jnp.float32, low / len(cuts), high / len(cuts))
        gain = gain * jnp.repeat(jnp.exp(steps), extent[axis_at] // blocks).reshape((-1,) + (1,) * (len(extent) - 1 - axis_at))
    return gain


def normal_values(rng, shape, width, limit, cuts=(), kind=jnp.bfloat16):
    loudness = block_levels(rng, shape, cuts, -0.22, 0.18) if cuts else 1.0
    values = jax.random.normal(rng, shape, jnp.float32) * width * loudness
    return jnp.minimum(jnp.maximum(values, -limit), limit).astype(kind)


def setup_inputs(seed: int = 0) -> dict:
    key_of = jax.random.split(jax.random.key(seed), 9)
    data = normal_values(key_of[0], (CHANNELS, SAMPLES), 1.0, 6.0, ((0, 8), (1, 64)))
    basis = normal_values(key_of[1], (NB, NT), NT ** -0.5, 0.75, (), jnp.float32)
    templates = normal_values(key_of[2], (UNITS, COEF), 3.0, 18.0, ((0, 512),), jnp.float32)
    spike_offset = draw_spike_offset(jax.random.fold_in(key_of[8], 71), 0)
    spike_unit = draw_spike_unit(jax.random.fold_in(key_of[8], 71), 0)
    spike_amp = jnp.clip(jnp.exp(math.log(2.0) - 1.3862944 * jax.random.uniform(key_of[5], (SPIKES,), jnp.float32) ** block_levels(key_of[5], (SPIKES,), ((0, 64),), -0.2, 0.2)), 0.5, 2.0)
    seg_count = draw_seg_count(jax.random.fold_in(key_of[8], 71), 0)
    neighbors = draw_neighbors(jax.random.fold_in(key_of[8], 71), 0)
    return dict(data=data, basis=basis, templates=templates, spike_offset=spike_offset, spike_unit=spike_unit, spike_amp=spike_amp, seg_count=seg_count, neighbors=neighbors)


prior_weight = 4.0


def reference(data, basis, templates, spike_offset, spike_unit, spike_amp, seg_count, neighbors):
    channel_count, sample_count = data.shape
    seg_total = seg_count.shape[0]
    seg_len = sample_count // seg_total
    slot_count = spike_offset.shape[0] // seg_total
    basis_count, tap_count = basis.shape
    half_width = (tap_count - 1) // 2
    ext_len = seg_len + 2 * half_width
    unit_count = templates.shape[0]
    nbr_width = neighbors.shape[1]
    live_mask = (jnp.arange(slot_count, dtype=jnp.int32)[None, :] < seg_count[:, None]).reshape(-1)
    weight = jnp.where(live_mask, spike_amp, jnp.zeros((), jnp.float32)).astype(jnp.float32)
    coef_all = templates.reshape(unit_count, basis_count, nbr_width)
    basis_low = basis.astype(jnp.bfloat16).astype(jnp.float32)
    basis_gram = jnp.dot(basis, basis.T, precision=lax.Precision.HIGHEST)
    zero_ints = jnp.zeros((1, slot_count), jnp.int32)
    zero_floats = jnp.zeros((1, slot_count), jnp.float32)
    offset_pad = jnp.concatenate([zero_ints, spike_offset.reshape(seg_total, slot_count), zero_ints], axis=0)
    unit_pad = jnp.concatenate([zero_ints, spike_unit.reshape(seg_total, slot_count), zero_ints], axis=0)
    weight_pad = jnp.concatenate([zero_floats, weight.reshape(seg_total, slot_count), zero_floats], axis=0)
    tap_index = jnp.arange(tap_count, dtype=jnp.int32)

    def one_segment(seg_index):
        model_sum = jnp.zeros((channel_count, ext_len), jnp.float32)
        for seg_shift in (-1, 0, 1):
            offsets = lax.dynamic_index_in_dim(offset_pad, seg_index + 1 + seg_shift, 0, keepdims=False)
            unit_ids = lax.dynamic_index_in_dim(unit_pad, seg_index + 1 + seg_shift, 0, keepdims=False)
            amp_rows = lax.dynamic_index_in_dim(weight_pad, seg_index + 1 + seg_shift, 0, keepdims=False)
            coef_low = (amp_rows[:, None, None] * coef_all[unit_ids]).astype(jnp.bfloat16).astype(jnp.float32)
            waves = jnp.einsum("sbj,bt->sjt", coef_low, basis_low, precision=lax.Precision.HIGHEST)
            columns = seg_shift * seg_len + offsets[:, None] + tap_index[None, :]
            columns = jnp.where((columns >= 0) & (columns < ext_len), columns, ext_len)
            chan_rows = neighbors[unit_ids]
            row_idx = jnp.broadcast_to(chan_rows[:, :, None], waves.shape)
            col_idx = jnp.broadcast_to(columns[:, None, :], waves.shape)
            model_sum = model_sum.at[row_idx, col_idx].add(waves, mode="drop")
        first_col = seg_index * seg_len
        left_part = lax.dynamic_slice(data, (jnp.int32(0), jnp.maximum(first_col - half_width, 0).astype(jnp.int32)), (channel_count, half_width))
        centre_part = lax.dynamic_slice(data, (jnp.int32(0), first_col.astype(jnp.int32)), (channel_count, seg_len))
        right_part = lax.dynamic_slice(data, (jnp.int32(0), jnp.minimum(first_col + seg_len, sample_count - half_width).astype(jnp.int32)), (channel_count, half_width))
        data_ext = jnp.concatenate([left_part, centre_part, right_part], axis=1).astype(jnp.float32)
        positions = first_col - half_width + jnp.arange(ext_len, dtype=jnp.int32)
        inside = (positions >= 0) & (positions < sample_count)
        res_ext = jnp.where(inside[None, :], data_ext - model_sum, jnp.zeros((), jnp.float32)).astype(jnp.bfloat16)
        offsets = lax.dynamic_index_in_dim(offset_pad, seg_index + 1, 0, keepdims=False)
        unit_ids = lax.dynamic_index_in_dim(unit_pad, seg_index + 1, 0, keepdims=False)
        amp_rows = lax.dynamic_index_in_dim(weight_pad, seg_index + 1, 0, keepdims=False)
        live_rows = (jnp.arange(slot_count, dtype=jnp.int32) < lax.dynamic_index_in_dim(seg_count, seg_index, 0, keepdims=False))
        chan_rows = neighbors[unit_ids]
        snippets = res_ext.astype(jnp.float32)[chan_rows[:, :, None], offsets[:, None, None] + tap_index[None, None, :]]
        projected = jnp.einsum("sjt,bt->sbj", snippets, basis_low, precision=lax.Precision.HIGHEST)
        own_term = amp_rows[:, None, None] * jnp.einsum("bk,skj->sbj", basis_gram, coef_all[unit_ids], precision=lax.Precision.HIGHEST)
        features = jnp.where(live_rows[:, None, None], projected + own_term, jnp.zeros((), jnp.float32))
        return res_ext[:, half_width:half_width + seg_len], features.reshape(slot_count, basis_count * nbr_width)

    res_all, features = lax.map(one_segment, jnp.arange(seg_total, dtype=jnp.int32))
    residual = jnp.transpose(res_all, (1, 0, 2)).reshape(channel_count, sample_count)
    features = features.reshape(seg_total * slot_count, basis_count * nbr_width)
    unit_sums = jax.ops.segment_sum(features, spike_unit, num_segments=unit_count)
    counts = jax.ops.segment_sum(live_mask.astype(jnp.float32), spike_unit, num_segments=unit_count)
    new_templates = (prior_weight * templates + unit_sums) / (prior_weight + counts[:, None])
    return residual, new_templates
```

```python
import functools

import jax
import jax.numpy as jnp
from jax import lax
from jax.experimental import pallas as pl
from jax.experimental.pallas import tpu as pltpu
from jax.sharding import PartitionSpec as P

MESH = pl.DeviceIdType.MESH
HI = lax.Precision.HIGHEST
BF = jnp.bfloat16
F32 = jnp.float32
I32 = jnp.int32
prior_weight = 4.0
LANES = 128
PER = 4
NBR = 32


def iota(shape, dim):
    return lax.broadcasted_iota(I32, shape, dim)


def dot(a, b, dims=((1,), (0,)), precision=None):
    return lax.dot_general(a, b, (dims, ((), ())), precision=precision, preferred_element_type=F32)


def one(mask, dtype=F32):
    return jnp.where(mask, 1.0, 0.0).astype(dtype)


def kernel(
    nt, nz, nc, group, taps,
    data, basis, templ, off, unit, amp, count, nbr,
    res_out, new_out,
    nbx, nbo, bp, mrow, msend, mrecv, hsend, hrecv, asrc, abuf, toep, shifted, maskc, placed, res,
    tbuf, ubuf, cbuf, csrc, dbuf,
    nsem, msem_s, msem_r, hsem_s, hsem_r, a1s, a1r, a2s, a2r, c1s, c1r, c2s, c2r,
):
    ny = nt // nz
    rb = nt // nc
    nrow = rb + 2
    row_units = nc * PER
    nb = basis.shape[0]
    half = (taps - 1) // 2
    quarter = group // 4
    shards = nrow * nc
    width = nb * LANES
    hw = width // 2
    t = lax.axis_index("tm")
    c = lax.axis_index("chan")
    y = t // nz
    z = t % nz
    band = t // rb
    at_low = (t % rb) == 0
    at_high = (t % rb) == rb - 1
    edge = jnp.logical_or(at_low, at_high)
    edge_band = jnp.where(at_low, (band + nc - 1) % nc, (band + 1) % nc)
    rr = (z + 2 * nz - (rb * c - 1) % nz) % nz
    gathers = rr < nrow
    src_row = (rb * c + nt - 1 + rr) % nt
    right = (t + 1) % nt
    left = (t + nt - 1) % nt

    barrier = pltpu.get_barrier_semaphore()

    def greet(tm, chan):
        pl.semaphore_signal(barrier, inc=1, device_id=(tm, chan), device_id_type=MESH)

    for d in range(1, nz):
        greet(y * nz + (z + d) % nz, c)
    greet(right, c)
    greet(left, c)
    n_greet = nz - 1 + 2 + jnp.where(edge, 2 * ny, ny) + jnp.where(gathers, nc, 0)
    own_main = band == c
    own_edge = jnp.logical_and(edge, edge_band == c)
    n_greet = n_greet - jnp.where(jnp.logical_or(own_main, own_edge), 1, 0)
    n_greet = n_greet - jnp.where(jnp.logical_and(gathers, src_row == t), 1, 0)
    for yy in range(ny):
        @pl.when(jnp.logical_or(yy != y, band != c))
        def _():
            greet(yy * nz + z, band)

        @pl.when(jnp.logical_and(edge, jnp.logical_or(yy != y, edge_band != c)))
        def _():
            greet(yy * nz + z, edge_band)
    for ch in range(nc):
        @pl.when(jnp.logical_and(gathers, jnp.logical_or(src_row != t, ch != c)))
        def _():
            greet(src_row, ch)

    lowest = (rb * c + nt - 1) % nt
    highest = (rb * c + rb) % nt
    copies = [
        pltpu.make_async_copy(nbr.at[pl.ds(lowest * row_units, row_units)], nbx.at[pl.ds(0, row_units)], nsem.at[0]),
        pltpu.make_async_copy(
            nbr.at[pl.ds(c * rb * row_units, rb * row_units)], nbx.at[pl.ds(row_units, rb * row_units)], nsem.at[1]
        ),
        pltpu.make_async_copy(
            nbr.at[pl.ds(highest * row_units, row_units)],
            nbx.at[pl.ds((rb + 1) * row_units, row_units)],
            nsem.at[2],
        ),
        pltpu.make_async_copy(nbr.at[pl.ds(t * row_units, row_units)], nbo, nsem.at[3]),
    ]
    for cp in copies:
        cp.start()

    mrow[...] = jnp.zeros_like(mrow)
    slots = off.shape[1]
    live = (iota((1, slots), 1) < count[...]).astype(F32)
    mrow[0:1, 0:slots] = unit[...].astype(F32)
    mrow[1:2, 0:slots] = off[...].astype(F32)
    mrow[2:3, 0:slots] = jnp.where(live > 0.0, amp[...], 0.0)
    mrow[3:4, 0:slots] = live
    meta = mrow[...]
    lane8 = iota((8, LANES), 1)
    row8 = iota((8, LANES), 0)
    go_right = jnp.where(t == nt - 1, 0.0, 1.0)
    go_left = jnp.where(t == 0, 0.0, 1.0)
    seg = data.shape[1]
    to_right = jnp.where(row8 == 1, meta - float(seg), jnp.where(row8 >= 2, meta * go_right, meta))
    to_left = jnp.where(row8 == 1, meta + float(seg), jnp.where(row8 >= 2, meta * go_left, meta))
    to_right = jnp.where(lane8 < slots, to_right, 0.0)
    to_left = jnp.where(lane8 < slots, to_left, 0.0)
    msend[0] = pltpu.roll(to_right, slots, 1)
    msend[1] = pltpu.roll(to_left, 2 * slots, 1)

    sel_i = iota((seg, 2 * LANES), 0)
    sel_j = iota((seg, 2 * LANES), 1)
    pack = jnp.zeros((quarter, 2 * LANES), F32)
    for k in range(4):
        to_r = (sel_j == sel_i - (seg - 32) + 32 * k) & (sel_i >= seg - 32)
        to_l = (sel_j == sel_i + 32 * k + LANES) & (sel_i < 32)
        pack = pack + dot(data[k * quarter:(k + 1) * quarter, :], one(to_r | to_l, BF))
    hsend[0] = pack[:, :LANES].astype(BF)
    hsend[1] = pack[:, LANES:].astype(BF)

    copies[3].wait()
    starts_own = nbo[:, 0:1]
    pick = iota((row_units, LANES), 0) == PER * c + iota((row_units, LANES), 1) // NBR
    s_lane = jnp.sum(jnp.where(pick, starts_own, 0), axis=0, keepdims=True)
    coef = nb * NBR
    turn = one(((iota((coef, LANES), 0) + s_lane - iota((coef, LANES), 1)) & (NBR - 1)) == 0)
    q_of = iota((8, coef), 1) // NBR
    b_of = iota((8, coef), 0)
    spread = jnp.concatenate([jnp.where(q_of == b_of, templ[u:u + 1, :], 0.0) for u in range(PER)], axis=0)
    turned = dot(spread, turn, precision=HI)
    lane_u = iota((8, LANES), 1) // NBR
    tblk = jnp.zeros((8, LANES), F32)
    for u in range(PER):
        tblk = tblk + jnp.where(lane_u == u, turned[8 * u:8 * u + 8, :], 0.0)
    asrc[...] = tblk

    pl.semaphore_wait(barrier, n_greet)

    def remote(src, dst, s, r, tm, chan):
        return pltpu.make_async_remote_copy(
            src_ref=src, dst_ref=dst, send_sem=s, recv_sem=r, device_id=(tm, chan), device_id_type=MESH
        )

    def block8(ref, i):
        return ref.at[pl.ds(pl.multiple_of(8 * i, 8), 8), :]

    def a1_copy(yy, e):
        return remote(asrc, block8(abuf, c), a1s.at[e * ny + yy], a1r.at[c], yy * nz + z, edge_band if e else band)

    for yy in range(ny):
        @pl.when(jnp.logical_or(yy != y, band != c))
        def _():
            a1_copy(yy, 0).start()

        @pl.when(jnp.logical_and(edge, jnp.logical_or(yy != y, edge_band != c)))
        def _():
            a1_copy(yy, 1).start()

    @pl.when(jnp.logical_or(own_main, own_edge))
    def _():
        block8(abuf, c)[...] = asrc[...]

    m_right = remote(msend.at[0], mrecv.at[0], msem_s.at[0], msem_r.at[0], right, c)
    m_left = remote(msend.at[1], mrecv.at[1], msem_s.at[1], msem_r.at[1], left, c)
    h_right = remote(hsend.at[0], hrecv.at[0], hsem_s.at[0], hsem_r.at[0], right, c)
    h_left = remote(hsend.at[1], hrecv.at[1], hsem_s.at[1], hsem_r.at[1], left, c)
    m_right.start()
    m_left.start()
    h_right.start()
    h_left.start()

    bp[...] = jnp.zeros_like(bp)
    bp[0:nb, 0:taps] = basis[...]
    span = 2 * LANES
    base = 66
    lane_s = iota((LANES, LANES), 1)

    def shifts(b):
        row = jnp.broadcast_to(bp[b:b + 1, :].astype(BF).astype(F32), (LANES, span))
        for r0 in (0, LANES):
            mid = pltpu.roll(row, (span - half - base + r0) % span, 1, stride=1, stride_axis=0)[:, :LANES]
            low = pltpu.roll(row, (span - half - base + 32 + r0) % span, 1, stride=1, stride_axis=0)[:, :LANES]
            high = pltpu.roll(row, (span - half - base - seg + 32 + r0) % span, 1, stride=1, stride_axis=0)[:, :LANES]
            side = jnp.where(lane_s < 32, low, jnp.where(lane_s < 64, high, 0.0))
            toep[b, r0:r0 + LANES, 0:LANES] = mid.astype(BF)
            toep[b, r0:r0 + LANES, LANES:span] = side.astype(BF)

    for b in range(nb):
        shifts(b)
    gram = dot(bp[...], bp[...], ((1,), (1,)), precision=HI)
    gram_t = dot(gram, tblk, precision=HI)

    @pl.when(gathers)
    def _():
        for ch in range(nc):
            @pl.when(jnp.logical_or(src_row != t, ch != c))
            def _():
                remote(asrc, block8(abuf, ch), a1s.at[0], a1r.at[ch], src_row, ch).wait_recv()
        rows = [abuf[pl.ds(b, nc, stride=8), :] for b in range(nb)]
        top = jnp.concatenate(rows[: nb // 2], axis=1)
        bottom = jnp.concatenate(rows[nb // 2:], axis=1)
        tbuf[rr] = jnp.concatenate([top, bottom], axis=0).astype(BF)
        for d in [nz // 2] + [s * k for k in range(nz // 2 - 1, 0, -1) for s in (1, -1)]:
            remote(tbuf.at[rr], tbuf.at[rr], a2s.at[d % nz], a2r.at[rr], y * nz + (z + d + nz) % nz, c).start()

    m_right.wait_recv()
    m_left.wait_recv()
    every = meta + mrecv[0] + mrecv[1]
    for cp in copies[:3]:
        cp.wait()
    units_x = nrow * row_units
    unit_lane = every[0:1, :].astype(I32)
    found = (iota((units_x, LANES), 0) + row_units * (rb * c - 1)) == unit_lane
    start_lane = jnp.sum(jnp.where(found, nbx[:, 0:1], 0), axis=0, keepdims=True) - group * c
    shard_lane = unit_lane // PER - nc * (rb * c - 1)
    sub_lane = unit_lane % PER
    live_lane = every[3:4, :]
    amp_lane = every[2:3, :]
    stack = jnp.where(row8 == 0, every[1:2, :] + float(base), 0.0)
    stack = jnp.where(row8 == 1, shard_lane.astype(F32), stack)
    stack = jnp.where(row8 == 2, sub_lane.astype(F32), stack)
    stack = jnp.where(row8 == 3, amp_lane, stack)
    stack = jnp.where(row8 == 4, start_lane.astype(F32), stack)
    cols = jnp.transpose(stack)
    pos_col = cols[:, 0:1].astype(I32)
    shard_col = cols[:, 1:2].astype(I32)
    sub_col = cols[:, 2:3].astype(I32)
    amp_col = cols[:, 3:4]
    start_col = cols[0:slots, 4:5].astype(I32)

    at_pos = one(pos_col == iota((LANES, span), 1), BF)
    for b in range(nb):
        shifted[b * LANES:(b + 1) * LANES, :] = dot(at_pos, toep[b]).astype(BF)
    maskc[...] = one(
        (iota((group, LANES), 0) >= start_lane) & (iota((group, LANES), 0) < start_lane + NBR), BF
    )
    own_mask = one((iota((slots, group), 1) >= start_col) & (iota((slots, group), 1) < start_col + NBR))
    shard_n = one(shard_col == iota((LANES, shards), 1), BF)
    n_shard = one(shard_lane == iota((shards, LANES), 0)) * live_lane
    lane_sub = iota((LANES, LANES), 1) // NBR
    weigh = jnp.where(lane_sub == sub_col, amp_col, 0.0)
    fold = one((iota((NBR, LANES), 1) & (NBR - 1)) == iota((NBR, LANES), 0), BF)
    spin = one((iota((LANES, LANES), 1) & (NBR - 1)) == (iota((LANES, LANES), 0) & (NBR - 1)), BF)
    sub_own = one(lane_sub == sub_col)[0:slots, :]

    l_i = iota((LANES, LANES), 1)
    tally_w = jnp.where(l_i < PER, one(l_i == sub_col), 0.0)
    tally_w = tally_w + jnp.where((l_i >= PER) & (l_i < 3 * PER), one((l_i & (PER - 1)) == sub_col) * amp_col, 0.0)
    tally_w = jnp.where(iota((LANES, LANES), 0) < slots, tally_w, 0.0)
    tally = dot(n_shard, tally_w, precision=HI)
    t_i = iota((shards, LANES), 0)
    tally = jnp.where((t_i >= nc) & (t_i < nc * (rb + 1)), tally, 0.0)
    coarse = tally.astype(BF).astype(F32)
    tally = jnp.where(iota((shards, LANES), 1) < 2 * PER, coarse, tally - coarse)

    h_right.wait_recv()
    h_left.wait_recv()
    un_i = iota((LANES, LANES), 0)
    un_j = iota((LANES, LANES), 1)
    wings = []
    for k in range(4):
        from_l = one((un_i == un_j + 32 * k) & (un_j < 32), BF)
        from_r = one((un_i == un_j - 32 + 32 * k) & (un_j >= 32) & (un_j < 64), BF)
        wings.append(dot(hrecv[0], from_l) + dot(hrecv[1], from_r))
    wing = jnp.concatenate(wings, axis=0)
    wing_lane = iota((group, LANES), 1)
    inside = ((wing_lane < 32) & (t > 0)) | ((wing_lane >= 32) & (wing_lane < 64) & (t < nt - 1))

    for k in range(nrow):
        zk = (rb * c + 2 * nz - 1 + k) % nz

        @pl.when(zk != z)
        def _():
            remote(tbuf.at[k], tbuf.at[k], a2s.at[0], a2r.at[k], y * nz + zk, c).wait_recv()
    blocks = [tbuf[k].astype(F32) for k in range(nrow)]
    t_top = jnp.concatenate([v[:nc] for v in blocks], axis=0).astype(BF)
    t_bottom = jnp.concatenate([v[nc:] for v in blocks], axis=0).astype(BF)
    chosen = [dot(shard_n, t_top), dot(shard_n, t_bottom)]
    for b in range(nb):
        part = chosen[b // (nb // 2)]
        b3 = b % (nb // 2)
        low = (part[:, b3 * LANES:(b3 + 1) * LANES] * weigh).astype(BF)
        lowt = dot(fold, low, ((1,), (1,))).astype(BF)
        placed[:, b * LANES:(b + 1) * LANES] = jnp.concatenate([lowt] * (group // NBR), axis=0) * maskc[...]
    model = dot(placed[...], shifted[...])
    centre = (data[...].astype(F32) - model[:, :LANES]).astype(BF)
    res_out[...] = centre
    res[:, 0:LANES] = centre
    res[:, LANES:span] = jnp.where(inside, wing - model[:, LANES:], 0.0).astype(BF)

    own_shift = jnp.concatenate([shifted[b * LANES:b * LANES + slots, :] for b in range(nb)], axis=0)
    along = dot(own_shift, res[...], ((1,), (1,)))
    own_all = jnp.concatenate([own_mask] * nb, axis=0)
    hit = along * own_all
    feat = hit[:, 0:LANES]
    for k in range(1, group // LANES):
        feat = feat + hit[:, k * LANES:(k + 1) * LANES]
    feat = dot(feat.astype(BF), spin)
    spread_w = jnp.concatenate([feat[b * slots:(b + 1) * slots, :] * sub_own for b in range(nb)], axis=1)
    sums = dot(n_shard[:, 0:slots].astype(BF), spread_w.astype(BF))
    for k in range(nrow):
        lo, hi = k * nc, (k + 1) * nc
        top = jnp.concatenate([sums[lo:hi, :hw], tally[lo:hi, :]], axis=1)
        bottom = jnp.concatenate([sums[lo:hi, hw:], jnp.zeros((nc, LANES), F32)], axis=1)
        ubuf[k] = jnp.concatenate([top, bottom], axis=0).astype(BF)
    for k in range(nrow):
        zk = (rb * c + 2 * nz - 1 + k) % nz

        @pl.when(zk != z)
        def _():
            remote(ubuf.at[k], cbuf.at[z], c1s.at[k], c1r.at[z], y * nz + zk, c).start()

        @pl.when(zk == z)
        def _():
            cbuf[z] = ubuf[k]

    to_edge = jnp.logical_or(rr == 0, rr == nrow - 1)
    slot_out = jnp.where(to_edge, ny, 0) + y

    def c2_copy(ch):
        return remote(block8(csrc, ch), block8(dbuf, slot_out), c2s.at[ch], c2r.at[slot_out], src_row, ch)

    @pl.when(jnp.logical_not(edge))
    def _():
        dbuf[8 * ny:16 * ny, :] = jnp.zeros((8 * ny, LANES), F32)

    @pl.when(gathers)
    def _():
        for d in range(1, nz):
            zd = (z + d) % nz
            remote(ubuf.at[0], cbuf.at[zd], c1s.at[0], c1r.at[zd], y * nz + zd, c).wait_recv()
        total = cbuf[0].astype(F32)
        for k in range(1, nz):
            total = total + cbuf[k].astype(F32)
        for b in range(nb):
            r0 = nc * (b // (nb // 2))
            l0 = LANES * (b % (nb // 2))
            csrc[pl.ds(b, nc, stride=8), :] = total[r0:r0 + nc, l0:l0 + LANES]
        csrc[pl.ds(nb, nc, stride=8), :] = total[:nc, hw:]
        csrc[pl.ds(nb + 1, nc, stride=8), :] = jnp.zeros((nc, LANES), F32)
        for ch in range(nc):
            mine = jnp.logical_and(src_row == t, ch == c)

            @pl.when(jnp.logical_not(mine))
            def _():
                c2_copy(ch).start()

            @pl.when(mine)
            def _():
                block8(dbuf, slot_out)[...] = csrc[8 * ch:8 * ch + 8, :]

    for yy in range(ny):
        @pl.when(jnp.logical_or(yy != y, band != c))
        def _():
            remote(block8(csrc, 0), block8(dbuf, yy), c2s.at[0], c2r.at[yy], yy * nz + z, band).wait_recv()

        @pl.when(jnp.logical_and(edge, jnp.logical_or(yy != y, edge_band != c)))
        def _():
            remote(
                block8(csrc, 0), block8(dbuf, ny + yy), c2s.at[0], c2r.at[ny + yy], yy * nz + z, edge_band
            ).wait_recv()
    got = dbuf[0:8, :]
    for k in range(1, 2 * ny):
        got = got + dbuf[8 * k:8 * k + 8, :]
    ex_i = iota((LANES, 2 * LANES), 0)
    ex_j = iota((LANES, 2 * LANES), 1)
    ex_u = (ex_j & (LANES - 1)) // NBR
    expand = one(((ex_j < LANES) & (ex_i == ex_u)) | ((ex_j >= LANES) & ((ex_i == ex_u + PER) | (ex_i == ex_u + 2 * PER))))
    wide = dot(got, expand, precision=HI)[nb:nb + 1, :]
    fresh = (prior_weight * tblk + got + wide[:, LANES:] * gram_t) / (prior_weight + wide[:, :LANES])
    split = jnp.concatenate([jnp.where(lane_u == u, fresh, 0.0) for u in range(PER)], axis=0)
    back = dot(split, turn, ((1,), (1,)), precision=HI)
    for u in range(PER):
        piece = jnp.where(q_of == b_of, back[8 * u:8 * u + 8, :], 0.0)
        new_out[u:u + 1, :] = jnp.sum(piece, axis=0, keepdims=True)

    for yy in range(ny):
        @pl.when(jnp.logical_or(yy != y, band != c))
        def _():
            a1_copy(yy, 0).wait_send()

        @pl.when(jnp.logical_and(edge, jnp.logical_or(yy != y, edge_band != c)))
        def _():
            a1_copy(yy, 1).wait_send()
    m_right.wait_send()
    m_left.wait_send()
    h_right.wait_send()
    h_left.wait_send()

    @pl.when(gathers)
    def _():
        for d in range(1, nz):
            remote(tbuf.at[rr], tbuf.at[rr], a2s.at[d], a2r.at[rr], y * nz + (z + d) % nz, c).wait_send()
        for ch in range(nc):
            @pl.when(jnp.logical_or(src_row != t, ch != c))
            def _():
                c2_copy(ch).wait_send()
    for k in range(nrow):
        zk = (rb * c + 2 * nz - 1 + k) % nz

        @pl.when(zk != z)
        def _():
            remote(ubuf.at[k], cbuf.at[z], c1s.at[k], c1r.at[z], y * nz + zk, c).wait_send()


def shards_fn(nt, nz, nc, data, basis, templates, spike_offset, spike_unit, spike_amp, seg_count, neighbors):
    group, seg = data.shape
    nb, taps = basis.shape
    slots = spike_offset.shape[0]
    ny = nt // nz
    rb = nt // nc
    nrow = rb + 2
    row_units = nc * PER
    width = nb * LANES
    dma = pltpu.SemaphoreType.DMA
    vmem = pl.BlockSpec(memory_space=pltpu.VMEM)
    return pl.pallas_call(
        functools.partial(kernel, nt, nz, nc, group, taps),
        out_shape=(
            jax.ShapeDtypeStruct(data.shape, BF),
            jax.ShapeDtypeStruct(templates.shape, F32),
        ),
        in_specs=[vmem] * 7 + [pl.BlockSpec(memory_space=pl.ANY)],
        out_specs=(vmem, vmem),
        scratch_shapes=[
            pltpu.VMEM((nrow * row_units, NBR), I32),
            pltpu.VMEM((row_units, NBR), I32),
            pltpu.VMEM((8, 2 * LANES), F32),
            pltpu.VMEM((8, LANES), F32),
            pltpu.VMEM((2, 8, LANES), F32),
            pltpu.VMEM((2, 8, LANES), F32),
            pltpu.VMEM((2, group // 4, LANES), BF),
            pltpu.VMEM((2, group // 4, LANES), BF),
            pltpu.VMEM((8, LANES), F32),
            pltpu.VMEM((8 * nc, LANES), F32),
            pltpu.VMEM((nb, 2 * LANES, 2 * LANES), BF),
            pltpu.VMEM((width, 2 * LANES), BF),
            pltpu.VMEM((group, LANES), BF),
            pltpu.VMEM((group, width), BF),
            pltpu.VMEM((group, 2 * LANES), BF),
            pltpu.VMEM((nrow, 2 * nc, width // 2), BF),
            pltpu.VMEM((nrow, 2 * nc, width // 2 + LANES), BF),
            pltpu.VMEM((nz, 2 * nc, width // 2 + LANES), BF),
            pltpu.VMEM((8 * nc, LANES), F32),
            pltpu.VMEM((16 * ny, LANES), F32),
            dma((4,)),
            dma((2,)), dma((2,)), dma((2,)), dma((2,)),
            dma((2 * ny,)), dma((nc,)),
            dma((nz,)), dma((nrow,)),
            dma((nrow,)), dma((nz,)),
            dma((nc,)), dma((2 * ny,)),
        ],
        compiler_params=pltpu.CompilerParams(collective_id=0, has_side_effects=True),
        name="step",
    )(
        data, basis, templates,
        spike_offset.reshape(1, slots), spike_unit.reshape(1, slots), spike_amp.reshape(1, slots),
        seg_count.reshape(1, 1), neighbors,
    )


def solution(mesh, nz=16):
    nt, nc = mesh.shape["tm"], mesh.shape["chan"]
    return jax.shard_map(
        functools.partial(shards_fn, nt, nz, nc),
        mesh=mesh,
        in_specs=(
            P("chan", "tm"),
            P(),
            P(("tm", "chan"), None),
            P("tm"),
            P("tm"),
            P("tm"),
            P("tm"),
            P(),
        ),
        out_specs=(P("chan", "tm"), P(("tm", "chan"), None)),
        check_vma=False,
    )
```

```python
import functools

import jax
import jax.numpy as jnp
from jax import lax
from jax.experimental import pallas as pl
from jax.experimental.pallas import tpu as pltpu
from jax.sharding import PartitionSpec as P

MESH = pl.DeviceIdType.MESH
HI = lax.Precision.HIGHEST
BF = jnp.bfloat16
F32 = jnp.float32
I32 = jnp.int32
prior_weight = 4.0
LANES = 128
PER = 4
NBR = 32


def iota(shape, dim):
    return lax.broadcasted_iota(I32, shape, dim)


def dot(a, b, dims=((1,), (0,)), precision=None):
    return lax.dot_general(a, b, (dims, ((), ())), precision=precision, preferred_element_type=F32)


def one(mask, dtype=F32):
    return jnp.where(mask, 1.0, 0.0).astype(dtype)


def kernel(
    nt, nz, nc, group, taps,
    data_h, basis_h, templ_h, off_h, unit_h, amp_h, count_h, nbr_h,
    res_h, new_out,
    data, basis, templ, off, unit, amp, count, nbv, res_out, bp, mrow, msend, mrecv, hsend, hrecv, asrc, abuf, toep, shifted, maskc, placed, res,
    tbuf, ubuf, rbuf, cbuf, csrc, dbuf,
    nsem, vouch, msem_s, msem_r, hsem_s, hsem_r, a1s, a1r, a2s, a2r, c1s, c1r, c1q, c2s, c2r,
):
    ny = nt // nz
    rb = nt // nc
    nrow = rb + 2
    row_units = nc * PER
    nb = basis_h.shape[0]
    half = (taps - 1) // 2
    hop = nz // 4
    quarter = group // 4
    shards = nrow * nc
    width = nb * LANES
    t = lax.axis_index("tm")
    c = lax.axis_index("chan")
    y = t // nz
    z = t % nz
    band = t // rb
    at_low = (t % rb) == 0
    at_high = (t % rb) == rb - 1
    edge = jnp.logical_or(at_low, at_high)
    edge_band = jnp.where(at_low, (band + nc - 1) % nc, (band + 1) % nc)
    rr = (z + 2 * nz - (rb * c - 1) % nz) % nz
    gathers = rr < nrow
    src_row = (rb * c + nt - 1 + rr) % nt
    right = (t + 1) % nt
    left = (t + nt - 1) % nt

    barrier = pltpu.get_barrier_semaphore()

    def greet(tm, chan):
        pl.semaphore_signal(barrier, inc=1, device_id=(tm, chan), device_id_type=MESH)

    for d in range(1, hop + 1):
        greet(y * nz + (z + d) % nz, c)
        greet(y * nz + (z + nz - d) % nz, c)
    greet(right, c)
    greet(left, c)
    n_greet = 2 * hop + 2 + jnp.where(edge, 2 * ny, ny) + jnp.where(gathers, nc, 0)
    own_main = band == c
    own_edge = jnp.logical_and(edge, edge_band == c)
    n_greet = n_greet - jnp.where(jnp.logical_or(own_main, own_edge), 1, 0)
    n_greet = n_greet - jnp.where(jnp.logical_and(gathers, src_row == t), 1, 0)
    for yy in range(ny):
        @pl.when(jnp.logical_or(yy != y, band != c))
        def _():
            greet(yy * nz + z, band)

        @pl.when(jnp.logical_and(edge, jnp.logical_or(yy != y, edge_band != c)))
        def _():
            greet(yy * nz + z, edge_band)
    for ch in range(nc):
        @pl.when(jnp.logical_and(gathers, jnp.logical_or(src_row != t, ch != c)))
        def _():
            greet(src_row, ch)

    def fetch(src, dst, i):
        return pltpu.make_async_copy(src, dst, nsem.at[i])

    small = [
        fetch(nbr_h.at[pl.ds(0, 8), :], nbv, 0),
        fetch(templ_h, templ, 1),
        fetch(off_h, off, 2),
        fetch(unit_h, unit, 3),
        fetch(amp_h, amp, 4),
        fetch(count_h, count, 5),
    ]
    for cp in small:
        cp.start()
    bp[...] = jnp.zeros_like(bp)
    get_data = fetch(data_h, data, 6)
    get_basis = fetch(basis_h, basis, 7)
    get_data.start()
    get_basis.start()
    mrow[...] = jnp.zeros_like(mrow)

    def parts(v):
        p0 = v.astype(BF)
        p1 = (v - p0.astype(F32)).astype(BF)
        p2 = (v - p0.astype(F32) - p1.astype(F32)).astype(BF)
        return jnp.concatenate([p0.astype(F32), p1.astype(F32), p2.astype(F32)], axis=0).astype(BF)

    def joined(v):
        n = v.shape[0] // 3
        return v[:n] + v[n:2 * n] + v[2 * n:]

    for cp in small:
        cp.wait()
    lane8 = iota((8, LANES), 1)
    row8 = iota((8, LANES), 0)
    lane_u = lane8 // NBR
    first = PER * (nc * t + c)
    mine = nbv[:, pl.ds(pl.multiple_of((first // LANES) * LANES, LANES), LANES)]
    mine = pltpu.roll(mine, (LANES - first % LANES) % LANES, 1)
    s_lane = jnp.zeros((1, LANES), I32)
    for u in range(PER):
        s_lane = s_lane + jnp.where(lane_u[0:1] == u, mine[0:1, u:u + 1], 0)
    coef = nb * NBR
    turn = one(((iota((coef, LANES), 0) + s_lane - iota((coef, LANES), 1)) & (NBR - 1)) == 0, BF)
    q_of = iota((8, coef), 1) // NBR
    b_of = iota((8, coef), 0)
    spread = jnp.concatenate([jnp.where(q_of == b_of, templ[u:u + 1, :], 0.0) for u in range(PER)], axis=0)
    turned = joined(dot(parts(spread), turn))
    tblk = jnp.zeros((8, LANES), F32)
    for u in range(PER):
        tblk = tblk + jnp.where(lane_u == u, turned[8 * u:8 * u + 8, :], 0.0)
    asrc[...] = tblk

    slots = off.shape[1]
    live = (iota((1, slots), 1) < count[...]).astype(F32)
    mrow[0:1, 0:slots] = unit[...].astype(F32)
    mrow[1:2, 0:slots] = off[...].astype(F32)
    mrow[2:3, 0:slots] = jnp.where(live > 0.0, amp[...], 0.0)
    mrow[3:4, 0:slots] = live
    meta = mrow[...]
    go_right = jnp.where(t == nt - 1, 0.0, 1.0)
    go_left = jnp.where(t == 0, 0.0, 1.0)
    seg = data_h.shape[1]
    to_right = jnp.where(row8 == 1, meta - float(seg), jnp.where(row8 >= 2, meta * go_right, meta))
    to_left = jnp.where(row8 == 1, meta + float(seg), jnp.where(row8 >= 2, meta * go_left, meta))
    to_right = jnp.where(lane8 < slots, to_right, 0.0)
    to_left = jnp.where(lane8 < slots, to_left, 0.0)
    msend[0] = pltpu.roll(to_right, slots, 1)
    msend[1] = pltpu.roll(to_left, 2 * slots, 1)

    pl.semaphore_wait(barrier, n_greet)
    for d in (hop, nz - hop):
        pl.semaphore_signal(vouch, inc=1, device_id=(y * nz + (z + d) % nz, c), device_id_type=MESH)

    def remote(src, dst, s, r, tm, chan):
        return pltpu.make_async_remote_copy(
            src_ref=src, dst_ref=dst, send_sem=s, recv_sem=r, device_id=(tm, chan), device_id_type=MESH
        )

    def block8(ref, i):
        return ref.at[pl.ds(pl.multiple_of(8 * i, 8), 8), :]

    def a1_copy(yy, e):
        return remote(asrc, block8(abuf, c), a1s.at[e * ny + yy], a1r.at[c], yy * nz + z, edge_band if e else band)

    for yy in range(ny):
        @pl.when(jnp.logical_or(yy != y, band != c))
        def _():
            a1_copy(yy, 0).start()

        @pl.when(jnp.logical_and(edge, jnp.logical_or(yy != y, edge_band != c)))
        def _():
            a1_copy(yy, 1).start()

    @pl.when(jnp.logical_or(own_main, own_edge))
    def _():
        block8(abuf, c)[...] = asrc[...]

    m_right = remote(msend.at[0], mrecv.at[0], msem_s.at[0], msem_r.at[0], right, c)
    m_left = remote(msend.at[1], mrecv.at[1], msem_s.at[1], msem_r.at[1], left, c)
    h_right = remote(hsend.at[0], hrecv.at[0], hsem_s.at[0], hsem_r.at[0], right, c)
    h_left = remote(hsend.at[1], hrecv.at[1], hsem_s.at[1], hsem_r.at[1], left, c)
    m_right.start()
    m_left.start()

    get_data.wait()
    sel_i = iota((seg, 2 * LANES), 0)
    sel_j = iota((seg, 2 * LANES), 1)
    pack = jnp.zeros((quarter, 2 * LANES), F32)
    for k in range(4):
        to_r = (sel_j == sel_i - (seg - 32) + 32 * k) & (sel_i >= seg - 32)
        to_l = (sel_j == sel_i + 32 * k + LANES) & (sel_i < 32)
        pack = pack + dot(data[k * quarter:(k + 1) * quarter, :], one(to_r | to_l, BF))
    hsend[0] = pack[:, :LANES].astype(BF)
    hsend[1] = pack[:, LANES:].astype(BF)

    h_right.start()
    h_left.start()

    get_basis.wait()
    bp[0:nb, 0:taps] = basis[...]
    span = 2 * LANES
    base = 66
    lane_s = iota((LANES, LANES), 1)

    def shifts(b):
        row = jnp.broadcast_to(bp[b:b + 1, :].astype(BF).astype(F32), (LANES, span))
        for r0 in (0, LANES):
            mid = pltpu.roll(row, (span - half - base + r0) % span, 1, stride=1, stride_axis=0)[:, :LANES]
            low = pltpu.roll(row, (span - half - base + 32 + r0) % span, 1, stride=1, stride_axis=0)[:, :LANES]
            high = pltpu.roll(row, (span - half - base - seg + 32 + r0) % span, 1, stride=1, stride_axis=0)[:, :LANES]
            side = jnp.where(lane_s < 32, low, jnp.where(lane_s < 64, high, 0.0))
            toep[b, r0:r0 + LANES, 0:LANES] = mid.astype(BF)
            toep[b, r0:r0 + LANES, LANES:span] = side.astype(BF)

    for b in range(nb):
        shifts(b)
    gram = dot(bp[...], bp[...], ((1,), (1,)), precision=HI)
    gram_t = dot(gram, tblk, precision=HI)

    pl.semaphore_wait(vouch, 2)

    @pl.when(gathers)
    def _():
        for ch in range(nc):
            @pl.when(jnp.logical_or(src_row != t, ch != c))
            def _():
                remote(asrc, block8(abuf, ch), a1s.at[0], a1r.at[ch], src_row, ch).wait_recv()
        rows = [abuf[pl.ds(b, nc, stride=8), :] for b in range(nb)]
        tbuf[rr] = jnp.concatenate(rows, axis=1).astype(BF)
        for d in [nz // 2] + [s * k for k in range(nz // 2 - 1, 0, -1) for s in (1, -1)]:
            remote(tbuf.at[rr], tbuf.at[rr], a2s.at[d % nz], a2r.at[rr], y * nz + (z + d + nz) % nz, c).start()

    m_right.wait_recv()
    m_left.wait_recv()
    every = meta + mrecv[0] + mrecv[1]
    unit_lane = every[0:1, :].astype(I32)
    shard_lane = unit_lane // PER - nc * (rb * c - 1)
    live_lane = every[3:4, :]
    stack = jnp.where(row8 == 1, every + float(base), jnp.where(row8 < 4, every, 0.0))
    cols = jnp.transpose(stack)
    unit_col = cols[:, 0:1].astype(I32)
    pos_col = cols[:, 1:2].astype(I32)
    amp_col = cols[:, 2:3]
    shard_col = unit_col // PER - nc * (rb * c - 1)
    sub_col = unit_col % PER
    n_tiles = nbv.shape[1] // LANES
    band_tiles = max(rb * row_units // LANES, 1)
    sum_start = jnp.zeros((LANES, LANES), I32)
    for k in range(min(band_tiles + 2, n_tiles)):
        tile = (c * rb * row_units // LANES - 1 + k + n_tiles) % n_tiles
        starts = nbv[:, pl.ds(pl.multiple_of(tile * LANES, LANES), LANES)][0:1]
        sum_start = sum_start + jnp.where(unit_col - tile * LANES == iota((LANES, LANES), 1), starts, 0)
    start_all = jnp.sum(sum_start.astype(F32), axis=1, keepdims=True) - float(group) * c.astype(F32)
    start_lane = jnp.transpose(jnp.broadcast_to(start_all, (LANES, LANES)))[0:1, :].astype(I32)
    start_col = start_all[0:slots].astype(I32)

    at_pos = one(pos_col == iota((LANES, span), 1), BF)
    for b in range(nb):
        shifted[b * LANES:(b + 1) * LANES, :] = dot(at_pos, toep[b]).astype(BF)
    maskc[...] = one(
        (iota((group, LANES), 0) >= start_lane) & (iota((group, LANES), 0) < start_lane + NBR), BF
    )
    own_mask = one((iota((slots, group), 1) >= start_col) & (iota((slots, group), 1) < start_col + NBR))
    shard_n = one(shard_col == iota((LANES, shards), 1), BF)
    n_shard = one(shard_lane == iota((shards, LANES), 0)) * live_lane
    lane_sub = iota((LANES, LANES), 1) // NBR
    weigh = jnp.where(lane_sub == sub_col, amp_col, 0.0)
    fold = one((iota((NBR, LANES), 1) & (NBR - 1)) == iota((NBR, LANES), 0), BF)
    spin = one((iota((LANES, LANES), 1) & (NBR - 1)) == (iota((LANES, LANES), 0) & (NBR - 1)), BF)
    sub_own = one(lane_sub == sub_col)[0:slots, :]

    l_i = iota((LANES, LANES), 1)
    tally_w = jnp.where(l_i < PER, one(l_i == sub_col), 0.0)
    tally_w = tally_w + jnp.where((l_i >= PER) & (l_i < 3 * PER), one((l_i & (PER - 1)) == sub_col) * amp_col, 0.0)
    tally_w = jnp.where(iota((LANES, LANES), 0) < slots, tally_w, 0.0)
    tally = dot(n_shard, tally_w, precision=HI)
    t_i = iota((shards, LANES), 0)
    tally = jnp.where((t_i >= nc) & (t_i < nc * (rb + 1)), tally, 0.0)
    coarse = tally.astype(BF).astype(F32)
    tally = jnp.where(iota((shards, LANES), 1) < 2 * PER, coarse, tally - coarse)

    h_right.wait_recv()
    h_left.wait_recv()
    un_i = iota((LANES, LANES), 0)
    un_j = iota((LANES, LANES), 1)
    wings = []
    for k in range(4):
        from_l = one((un_i == un_j + 32 * k) & (un_j < 32), BF)
        from_r = one((un_i == un_j - 32 + 32 * k) & (un_j >= 32) & (un_j < 64), BF)
        wings.append(dot(hrecv[0], from_l) + dot(hrecv[1], from_r))
    wing = jnp.concatenate(wings, axis=0)
    wing_lane = iota((group, LANES), 1)
    inside = ((wing_lane < 32) & (t > 0)) | ((wing_lane >= 32) & (wing_lane < 64) & (t < nt - 1))

    for k in range(nrow):
        zk = (rb * c + 2 * nz - 1 + k) % nz

        @pl.when(zk != z)
        def _():
            remote(tbuf.at[k], tbuf.at[k], a2s.at[0], a2r.at[k], y * nz + zk, c).wait_recv()
    blocks = [tbuf[k].astype(F32) for k in range(nrow)]
    chosen = dot(shard_n, jnp.concatenate(blocks, axis=0).astype(BF))
    for b in range(nb):
        low = (chosen[:, b * LANES:(b + 1) * LANES] * weigh).astype(BF)
        lowt = dot(fold, low, ((1,), (1,))).astype(BF)
        placed[:, b * LANES:(b + 1) * LANES] = jnp.concatenate([lowt] * (group // NBR), axis=0) * maskc[...]
    model = dot(placed[...], shifted[...])
    centre = (data[...].astype(F32) - model[:, :LANES]).astype(BF)
    res_out[...] = centre
    put_res = fetch(res_out, res_h, 8)
    put_res.start()
    res[:, 0:LANES] = centre
    res[:, LANES:span] = jnp.where(inside, wing - model[:, LANES:], 0.0).astype(BF)

    own_shift = jnp.concatenate([shifted[b * LANES:b * LANES + slots, :] for b in range(nb)], axis=0)
    along = dot(own_shift, res[...], ((1,), (1,)))
    own_all = jnp.concatenate([own_mask] * nb, axis=0)
    hit = along * own_all
    feat = hit[:, 0:LANES]
    for k in range(1, group // LANES):
        feat = feat + hit[:, k * LANES:(k + 1) * LANES]
    feat = dot(feat.astype(BF), spin)
    spread_w = jnp.concatenate([feat[b * slots:(b + 1) * slots, :] * sub_own for b in range(nb)], axis=1)
    sums = dot(n_shard[:, 0:slots].astype(BF), spread_w.astype(BF))
    for k in range(nrow):
        lo, hi = k * nc, (k + 1) * nc
        ubuf[k] = jnp.concatenate([sums[lo:hi, :], tally[lo:hi, :]], axis=1).astype(BF)

    def z_of(k):
        return (rb * c + 2 * nz - 1 + k) % nz

    def to_relay(f):
        for k in range(nrow):
            dist = (z - z_of(k) + nz) % nz

            @pl.when(jnp.logical_and(dist > hop, dist <= 2 * hop))
            def _():
                at = y * nz + (z_of(k) + hop) % nz
                f(remote(ubuf.at[k], rbuf.at[dist - hop - 1], c1s.at[k], c1q.at[dist - hop - 1], at, c))

            @pl.when(jnp.logical_and(dist > 2 * hop, dist < 3 * hop))
            def _():
                at = y * nz + (z_of(k) + nz - hop) % nz
                i = 4 * hop - 1 - dist
                f(remote(ubuf.at[k], rbuf.at[i], c1s.at[k], c1q.at[i], at, c))

    def near_slot(dist):
        return jnp.where(dist <= hop, dist - 1, dist - 2 * hop)

    def to_gatherer(f):
        for k in range(nrow):
            dist = (z - z_of(k) + nz) % nz

            @pl.when(jnp.logical_or(jnp.logical_and(dist >= 1, dist < hop), dist > 3 * hop))
            def _():
                i = near_slot(dist)
                f(remote(ubuf.at[k], cbuf.at[i], c1s.at[k], c1r.at[i], y * nz + z_of(k), c))

    relays = ((hop, 0, hop), (3 * hop, hop, 2 * hop - 1))

    def relay_copy(dist):
        zt = (z - dist + nz) % nz
        k = (zt + 2 * nz - (rb * c - 1) % nz) % nz
        i = hop - 1 if dist == hop else hop
        return k, remote(ubuf.at[k], cbuf.at[i], c1s.at[k], c1r.at[i], y * nz + zt, c)

    to_relay(lambda cp: cp.start())
    to_gatherer(lambda cp: cp.start())
    for dist, lo, hi in relays:
        k, out = relay_copy(dist)

        @pl.when(k < nrow)
        def _():
            for j in range(lo, hi):
                remote(ubuf.at[0], rbuf.at[j], c1s.at[0], c1q.at[j], y * nz + (z + 1) % nz, c).wait_recv()
            part = ubuf[k].astype(F32)
            for j in range(lo, hi):
                part = part + rbuf[j].astype(F32)
            ubuf[k] = part.astype(BF)
            out.start()

    to_edge = jnp.logical_or(rr == 0, rr == nrow - 1)
    slot_out = jnp.where(to_edge, ny, 0) + y

    def c2_copy(ch):
        return remote(block8(csrc, ch), block8(dbuf, slot_out), c2s.at[ch], c2r.at[slot_out], src_row, ch)

    @pl.when(jnp.logical_not(edge))
    def _():
        dbuf[8 * ny:16 * ny, :] = jnp.zeros((8 * ny, LANES), F32)

    @pl.when(gathers)
    def _():
        for i in [j for j in range(2 * hop) if j not in (hop - 1, hop)] + [hop - 1, hop]:
            remote(ubuf.at[0], cbuf.at[i], c1s.at[0], c1r.at[i], y * nz + (z + 1) % nz, c).wait_recv()
        total = ubuf[rr].astype(F32)
        for k in range(2 * hop):
            total = total + cbuf[k].astype(F32)
        for b in range(nb + 1):
            csrc[pl.ds(b, nc, stride=8), :] = total[:, b * LANES:(b + 1) * LANES]
        csrc[pl.ds(nb + 1, nc, stride=8), :] = jnp.zeros((nc, LANES), F32)
        for ch in range(nc):
            is_own = jnp.logical_and(src_row == t, ch == c)

            @pl.when(jnp.logical_not(is_own))
            def _():
                c2_copy(ch).start()

            @pl.when(is_own)
            def _():
                block8(dbuf, slot_out)[...] = csrc[8 * ch:8 * ch + 8, :]

    for yy in range(ny):
        @pl.when(jnp.logical_or(yy != y, band != c))
        def _():
            remote(block8(csrc, 0), block8(dbuf, yy), c2s.at[0], c2r.at[yy], yy * nz + z, band).wait_recv()

        @pl.when(jnp.logical_and(edge, jnp.logical_or(yy != y, edge_band != c)))
        def _():
            remote(
                block8(csrc, 0), block8(dbuf, ny + yy), c2s.at[0], c2r.at[ny + yy], yy * nz + z, edge_band
            ).wait_recv()
    got = dbuf[0:8, :]
    for k in range(1, 2 * ny):
        got = got + dbuf[8 * k:8 * k + 8, :]
    tail = got[nb:nb + 1, :]
    number = jnp.zeros((1, LANES), F32)
    weight = jnp.zeros((1, LANES), F32)
    for u in range(PER):
        here = lane_u[0:1] == u
        number = number + jnp.where(here, tail[:, u:u + 1], 0.0)
        weight = weight + jnp.where(here, tail[:, PER + u:PER + u + 1] + tail[:, 2 * PER + u:2 * PER + u + 1], 0.0)
    fresh = (prior_weight * tblk + got + weight * gram_t) / (prior_weight + number)
    split = jnp.concatenate([jnp.where(lane_u == u, fresh, 0.0) for u in range(PER)], axis=0)
    back = joined(dot(parts(split), turn, ((1,), (1,))))
    for u in range(PER):
        piece = jnp.where(q_of == b_of, back[8 * u:8 * u + 8, :], 0.0)
        new_out[u:u + 1, :] = jnp.sum(piece, axis=0, keepdims=True)

    for yy in range(ny):
        @pl.when(jnp.logical_or(yy != y, band != c))
        def _():
            a1_copy(yy, 0).wait_send()

        @pl.when(jnp.logical_and(edge, jnp.logical_or(yy != y, edge_band != c)))
        def _():
            a1_copy(yy, 1).wait_send()
    m_right.wait_send()
    m_left.wait_send()
    h_right.wait_send()
    h_left.wait_send()

    @pl.when(gathers)
    def _():
        for d in range(1, nz):
            remote(tbuf.at[rr], tbuf.at[rr], a2s.at[d], a2r.at[rr], y * nz + (z + d) % nz, c).wait_send()
        for ch in range(nc):
            @pl.when(jnp.logical_or(src_row != t, ch != c))
            def _():
                c2_copy(ch).wait_send()
    to_relay(lambda cp: cp.wait_send())
    to_gatherer(lambda cp: cp.wait_send())
    for dist, lo, hi in relays:
        k, out = relay_copy(dist)

        @pl.when(k < nrow)
        def _():
            out.wait_send()
    put_res.wait()


def shards_fn(nt, nz, nc, data, basis, templates, spike_offset, spike_unit, spike_amp, seg_count, neighbors):
    group, seg = data.shape
    nb, taps = basis.shape
    slots = spike_offset.shape[0]
    ny = nt // nz
    rb = nt // nc
    nrow = rb + 2
    row_units = nc * PER
    width = nb * LANES
    dma = pltpu.SemaphoreType.DMA
    vmem = pl.BlockSpec(memory_space=pltpu.VMEM)
    hbm = pl.BlockSpec(memory_space=pl.ANY)
    hop = nz // 4
    return pl.pallas_call(
        functools.partial(kernel, nt, nz, nc, group, taps),
        out_shape=(
            jax.ShapeDtypeStruct(data.shape, BF),
            jax.ShapeDtypeStruct(templates.shape, F32),
        ),
        in_specs=[hbm] * 8,
        out_specs=(hbm, vmem),
        scratch_shapes=[
            pltpu.VMEM(data.shape, BF),
            pltpu.VMEM(basis.shape, F32),
            pltpu.VMEM(templates.shape, F32),
            pltpu.VMEM((1, slots), I32),
            pltpu.VMEM((1, slots), I32),
            pltpu.VMEM((1, slots), F32),
            pltpu.VMEM((1, 1), I32),
            pltpu.VMEM((8, neighbors.shape[0]), I32),
            pltpu.VMEM(data.shape, BF),
            pltpu.VMEM((8, 2 * LANES), F32),
            pltpu.VMEM((8, LANES), F32),
            pltpu.VMEM((2, 8, LANES), F32),
            pltpu.VMEM((2, 8, LANES), F32),
            pltpu.VMEM((2, group // 4, LANES), BF),
            pltpu.VMEM((2, group // 4, LANES), BF),
            pltpu.VMEM((8, LANES), F32),
            pltpu.VMEM((8 * nc, LANES), F32),
            pltpu.VMEM((nb, 2 * LANES, 2 * LANES), BF),
            pltpu.VMEM((width, 2 * LANES), BF),
            pltpu.VMEM((group, LANES), BF),
            pltpu.VMEM((group, width), BF),
            pltpu.VMEM((group, 2 * LANES), BF),
            pltpu.VMEM((nrow, nc, width), BF),
            pltpu.VMEM((nrow, nc, width + LANES), BF),
            pltpu.VMEM((2 * hop - 1, nc, width + LANES), BF),
            pltpu.VMEM((2 * hop, nc, width + LANES), BF),
            pltpu.VMEM((8 * nc, LANES), F32),
            pltpu.VMEM((16 * ny, LANES), F32),
            dma((9,)), pltpu.SemaphoreType.REGULAR,
            dma((2,)), dma((2,)), dma((2,)), dma((2,)),
            dma((2 * ny,)), dma((nc,)),
            dma((nz,)), dma((nrow,)),
            dma((nrow,)), dma((2 * hop,)), dma((2 * hop - 1,)),
            dma((nc,)), dma((2 * ny,)),
        ],
        compiler_params=pltpu.CompilerParams(collective_id=0, has_side_effects=True),
        name="step",
    )(
        data, basis, templates,
        spike_offset.reshape(1, slots), spike_unit.reshape(1, slots), spike_amp.reshape(1, slots),
        seg_count.reshape(1, 1), neighbors.T,
    )


def solution(mesh, nz=16):
    nt, nc = mesh.shape["tm"], mesh.shape["chan"]
    return jax.shard_map(
        functools.partial(shards_fn, nt, nz, nc),
        mesh=mesh,
        in_specs=(
            P("chan", "tm"),
            P(),
            P(("tm", "chan"), None),
            P("tm"),
            P("tm"),
            P("tm"),
            P("tm"),
            P(),
        ),
        out_specs=(P("chan", "tm"), P(("tm", "chan"), None)),
        check_vma=False,
    )
```

```python
import functools

import jax
import jax.numpy as jnp
from jax import lax
from jax.experimental import pallas as pl
from jax.experimental.pallas import tpu as pltpu
from jax.sharding import PartitionSpec as P

MESH = pl.DeviceIdType.MESH
HI = lax.Precision.HIGHEST
BF = jnp.bfloat16
F32 = jnp.float32
I32 = jnp.int32
prior_weight = 4.0
LANES = 128
PER = 4
NBR = 32


def iota(shape, dim):
    return lax.broadcasted_iota(I32, shape, dim)


def dot(a, b, dims=((1,), (0,)), precision=None):
    return lax.dot_general(a, b, (dims, ((), ())), precision=precision, preferred_element_type=F32)


def one(mask, dtype=F32):
    return jnp.where(mask, 1.0, 0.0).astype(dtype)


def kernel(
    nt, nz, nc, group, taps,
    data_h, basis_h, templ_h, off_h, unit_h, amp_h, count_h, nbr_h,
    res_h, new_out,
    data, basis, templ, off, unit, amp, count, nbv, res_out, bp, mrow, msend, mrecv, hsend, hrecv, asrc, abuf, toep, shifted, maskc, placed, res,
    tbuf, ubuf, rbuf, cbuf, csrc, dbuf,
    nsem, vouch, msem_s, msem_r, hsem_s, hsem_r, a1s, a1r, a2s, a2r, c1s, c1r, c1q, c2s, c2r,
):
    ny = nt // nz
    rb = nt // nc
    nrow = rb + 2
    row_units = nc * PER
    nb = basis_h.shape[0]
    half = (taps - 1) // 2
    hop = nz // 4
    quarter = group // 4
    shards = nrow * nc
    width = nb * LANES
    t = lax.axis_index("tm")
    c = lax.axis_index("chan")
    y = t // nz
    z = t % nz
    band = t // rb
    at_low = (t % rb) == 0
    at_high = (t % rb) == rb - 1
    edge = jnp.logical_or(at_low, at_high)
    edge_band = jnp.where(at_low, (band + nc - 1) % nc, (band + 1) % nc)
    rr = (z + 2 * nz - (rb * c - 1) % nz) % nz
    gathers = rr < nrow
    src_row = (rb * c + nt - 1 + rr) % nt
    right = (t + 1) % nt
    left = (t + nt - 1) % nt

    barrier = pltpu.get_barrier_semaphore()

    def greet(tm, chan):
        pl.semaphore_signal(barrier, inc=1, device_id=(tm, chan), device_id_type=MESH)

    for d in range(1, hop + 1):
        greet(y * nz + (z + d) % nz, c)
        greet(y * nz + (z + nz - d) % nz, c)
    greet(right, c)
    greet(left, c)
    n_greet = 2 * hop + 2 + jnp.where(edge, 2 * ny, ny) + jnp.where(gathers, nc, 0)
    own_main = band == c
    own_edge = jnp.logical_and(edge, edge_band == c)
    n_greet = n_greet - jnp.where(jnp.logical_or(own_main, own_edge), 1, 0)
    n_greet = n_greet - jnp.where(jnp.logical_and(gathers, src_row == t), 1, 0)
    for yy in range(ny):
        @pl.when(jnp.logical_or(yy != y, band != c))
        def _():
            greet(yy * nz + z, band)

        @pl.when(jnp.logical_and(edge, jnp.logical_or(yy != y, edge_band != c)))
        def _():
            greet(yy * nz + z, edge_band)
    for ch in range(nc):
        @pl.when(jnp.logical_and(gathers, jnp.logical_or(src_row != t, ch != c)))
        def _():
            greet(src_row, ch)

    def fetch(src, dst, i):
        return pltpu.make_async_copy(src, dst, nsem.at[i])

    small = [
        fetch(nbr_h.at[pl.ds(0, 8), :], nbv, 0),
        fetch(templ_h, templ, 1),
        fetch(off_h, off, 2),
        fetch(unit_h, unit, 3),
        fetch(amp_h, amp, 4),
        fetch(count_h, count, 5),
    ]
    for cp in small:
        cp.start()
    bp[...] = jnp.zeros_like(bp)
    get_data = fetch(data_h, data, 6)
    get_basis = fetch(basis_h, basis, 7)
    get_data.start()
    get_basis.start()
    mrow[...] = jnp.zeros_like(mrow)

    def parts(v):
        p0 = v.astype(BF)
        p1 = (v - p0.astype(F32)).astype(BF)
        p2 = (v - p0.astype(F32) - p1.astype(F32)).astype(BF)
        return jnp.concatenate([p0.astype(F32), p1.astype(F32), p2.astype(F32)], axis=0).astype(BF)

    def joined(v):
        n = v.shape[0] // 3
        return v[:n] + v[n:2 * n] + v[2 * n:]

    for cp in small:
        cp.wait()
    lane8 = iota((8, LANES), 1)
    row8 = iota((8, LANES), 0)
    lane_u = lane8 // NBR
    first = PER * (nc * t + c)
    mine = nbv[:, pl.ds(pl.multiple_of((first // LANES) * LANES, LANES), LANES)]
    mine = pltpu.roll(mine, (LANES - first % LANES) % LANES, 1)
    s_lane = jnp.zeros((1, LANES), I32)
    for u in range(PER):
        s_lane = s_lane + jnp.where(lane_u[0:1] == u, mine[0:1, u:u + 1], 0)
    coef = nb * NBR
    turn = one(((iota((coef, LANES), 0) + s_lane - iota((coef, LANES), 1)) & (NBR - 1)) == 0, BF)
    q_of = iota((8, coef), 1) // NBR
    b_of = iota((8, coef), 0)
    spread = jnp.concatenate([jnp.where(q_of == b_of, templ[u:u + 1, :], 0.0) for u in range(PER)], axis=0)
    turned = joined(dot(parts(spread), turn))
    tblk = jnp.zeros((8, LANES), F32)
    for u in range(PER):
        tblk = tblk + jnp.where(lane_u == u, turned[8 * u:8 * u + 8, :], 0.0)
    asrc[...] = tblk

    slots = off.shape[1]
    live = (iota((1, slots), 1) < count[...]).astype(F32)
    mrow[0:1, 0:slots] = unit[...].astype(F32)
    mrow[1:2, 0:slots] = off[...].astype(F32)
    mrow[2:3, 0:slots] = jnp.where(live > 0.0, amp[...], 0.0)
    mrow[3:4, 0:slots] = live
    meta = mrow[...]
    go_right = jnp.where(t == nt - 1, 0.0, 1.0)
    go_left = jnp.where(t == 0, 0.0, 1.0)
    seg = data_h.shape[1]
    to_right = jnp.where(row8 == 1, meta - float(seg), jnp.where(row8 >= 2, meta * go_right, meta))
    to_left = jnp.where(row8 == 1, meta + float(seg), jnp.where(row8 >= 2, meta * go_left, meta))
    to_right = jnp.where(lane8 < slots, to_right, 0.0)
    to_left = jnp.where(lane8 < slots, to_left, 0.0)
    msend[0] = pltpu.roll(to_right, slots, 1)
    msend[1] = pltpu.roll(to_left, 2 * slots, 1)

    pl.semaphore_wait(barrier, n_greet)
    for d in (hop, nz - hop):
        pl.semaphore_signal(vouch, inc=1, device_id=(y * nz + (z + d) % nz, c), device_id_type=MESH)

    def remote(src, dst, s, r, tm, chan):
        return pltpu.make_async_remote_copy(
            src_ref=src, dst_ref=dst, send_sem=s, recv_sem=r, device_id=(tm, chan), device_id_type=MESH
        )

    def block8(ref, i):
        return ref.at[pl.ds(pl.multiple_of(8 * i, 8), 8), :]

    def a1_copy(yy, e):
        return remote(asrc, block8(abuf, c), a1s.at[e * ny + yy], a1r.at[c], yy * nz + z, edge_band if e else band)

    for yy in range(ny):
        @pl.when(jnp.logical_or(yy != y, band != c))
        def _():
            a1_copy(yy, 0).start()

        @pl.when(jnp.logical_and(edge, jnp.logical_or(yy != y, edge_band != c)))
        def _():
            a1_copy(yy, 1).start()

    @pl.when(jnp.logical_or(own_main, own_edge))
    def _():
        block8(abuf, c)[...] = asrc[...]

    m_right = remote(msend.at[0], mrecv.at[0], msem_s.at[0], msem_r.at[0], right, c)
    m_left = remote(msend.at[1], mrecv.at[1], msem_s.at[1], msem_r.at[1], left, c)
    h_right = remote(hsend.at[0], hrecv.at[0], hsem_s.at[0], hsem_r.at[0], right, c)
    h_left = remote(hsend.at[1], hrecv.at[1], hsem_s.at[1], hsem_r.at[1], left, c)
    m_right.start()
    m_left.start()

    get_data.wait()
    sel_i = iota((seg, 2 * LANES), 0)
    sel_j = iota((seg, 2 * LANES), 1)
    pack = jnp.zeros((quarter, 2 * LANES), F32)
    for k in range(4):
        to_r = (sel_j == sel_i - (seg - 32) + 32 * k) & (sel_i >= seg - 32)
        to_l = (sel_j == sel_i + 32 * k + LANES) & (sel_i < 32)
        pack = pack + dot(data[k * quarter:(k + 1) * quarter, :], one(to_r | to_l, BF))
    hsend[0] = pack[:, :LANES].astype(BF)
    hsend[1] = pack[:, LANES:].astype(BF)

    h_right.start()
    h_left.start()

    get_basis.wait()
    bp[0:nb, 0:taps] = basis[...]
    span = 2 * LANES
    base = 66
    lane_s = iota((LANES, LANES), 1)

    def shifts(b):
        row = jnp.broadcast_to(bp[b:b + 1, :].astype(BF).astype(F32), (LANES, span))
        for r0 in (0, LANES):
            mid = pltpu.roll(row, (span - half - base + r0) % span, 1, stride=1, stride_axis=0)[:, :LANES]
            low = pltpu.roll(row, (span - half - base + 32 + r0) % span, 1, stride=1, stride_axis=0)[:, :LANES]
            high = pltpu.roll(row, (span - half - base - seg + 32 + r0) % span, 1, stride=1, stride_axis=0)[:, :LANES]
            side = jnp.where(lane_s < 32, low, jnp.where(lane_s < 64, high, 0.0))
            toep[b, r0:r0 + LANES, 0:LANES] = mid.astype(BF)
            toep[b, r0:r0 + LANES, LANES:span] = side.astype(BF)

    for b in range(nb):
        shifts(b)
    gram = dot(bp[...], bp[...], ((1,), (1,)), precision=HI)
    gram_t = dot(gram, tblk, precision=HI)

    pl.semaphore_wait(vouch, 2)

    @pl.when(gathers)
    def _():
        for ch in range(nc):
            @pl.when(jnp.logical_or(src_row != t, ch != c))
            def _():
                remote(asrc, block8(abuf, ch), a1s.at[0], a1r.at[ch], src_row, ch).wait_recv()
        rows = [abuf[pl.ds(b, nc, stride=8), :] for b in range(nb)]
        tbuf[rr] = jnp.concatenate(rows, axis=1).astype(BF)
        for d in [nz // 2] + [s * k for k in range(nz // 2 - 1, 0, -1) for s in (1, -1)]:
            remote(tbuf.at[rr], tbuf.at[rr], a2s.at[d % nz], a2r.at[rr], y * nz + (z + d + nz) % nz, c).start()

    m_right.wait_recv()
    m_left.wait_recv()
    every = meta + mrecv[0] + mrecv[1]
    unit_lane = every[0:1, :].astype(I32)
    shard_lane = unit_lane // PER - nc * (rb * c - 1)
    live_lane = every[3:4, :]
    stack = jnp.where(row8 == 1, every + float(base), jnp.where(row8 < 4, every, 0.0))
    cols = jnp.transpose(stack)
    unit_col = cols[:, 0:1].astype(I32)
    pos_col = cols[:, 1:2].astype(I32)
    amp_col = cols[:, 2:3]
    shard_col = unit_col // PER - nc * (rb * c - 1)
    sub_col = unit_col % PER
    n_tiles = nbv.shape[1] // LANES
    band_tiles = max(rb * row_units // LANES, 1)
    sum_start = jnp.zeros((LANES, LANES), I32)
    for k in range(min(band_tiles + 2, n_tiles)):
        tile = (c * rb * row_units // LANES - 1 + k + n_tiles) % n_tiles
        starts = nbv[:, pl.ds(pl.multiple_of(tile * LANES, LANES), LANES)][0:1]
        sum_start = sum_start + jnp.where(unit_col - tile * LANES == iota((LANES, LANES), 1), starts, 0)
    start_all = jnp.sum(sum_start.astype(F32), axis=1, keepdims=True) - float(group) * c.astype(F32)
    start_lane = jnp.transpose(jnp.broadcast_to(start_all, (LANES, LANES)))[0:1, :].astype(I32)
    start_col = start_all[0:slots].astype(I32)

    at_pos = one(pos_col == iota((LANES, span), 1), BF)
    for b in range(nb):
        shifted[b * LANES:(b + 1) * LANES, :] = dot(at_pos, toep[b]).astype(BF)
    maskc[...] = one(
        (iota((group, LANES), 0) >= start_lane) & (iota((group, LANES), 0) < start_lane + NBR), BF
    )
    own_mask = one((iota((slots, group), 1) >= start_col) & (iota((slots, group), 1) < start_col + NBR))
    shard_n = one(shard_col == iota((LANES, shards), 1), BF)
    n_shard = one(shard_lane == iota((shards, LANES), 0)) * live_lane
    lane_sub = iota((LANES, LANES), 1) // NBR
    weigh = jnp.where(lane_sub == sub_col, amp_col, 0.0)
    fold = one((iota((NBR, LANES), 1) & (NBR - 1)) == iota((NBR, LANES), 0), BF)
    spin = one((iota((LANES, LANES), 1) & (NBR - 1)) == (iota((LANES, LANES), 0) & (NBR - 1)), BF)
    sub_own = one(lane_sub == sub_col)[0:slots, :]

    l_i = iota((LANES, LANES), 1)
    tally_w = jnp.where(l_i < PER, one(l_i == sub_col), 0.0)
    tally_w = tally_w + jnp.where((l_i >= PER) & (l_i < 3 * PER), one((l_i & (PER - 1)) == sub_col) * amp_col, 0.0)
    tally_w = jnp.where(iota((LANES, LANES), 0) < slots, tally_w, 0.0)
    tally = dot(n_shard, tally_w, precision=HI)
    t_i = iota((shards, LANES), 0)
    tally = jnp.where((t_i >= nc) & (t_i < nc * (rb + 1)), tally, 0.0)
    coarse = tally.astype(BF).astype(F32)
    tally = jnp.where(iota((shards, LANES), 1) < 2 * PER, coarse, tally - coarse)

    h_right.wait_recv()
    h_left.wait_recv()
    un_i = iota((LANES, LANES), 0)
    un_j = iota((LANES, LANES), 1)
    wings = []
    for k in range(4):
        from_l = one((un_i == un_j + 32 * k) & (un_j < 32), BF)
        from_r = one((un_i == un_j - 32 + 32 * k) & (un_j >= 32) & (un_j < 64), BF)
        wings.append(dot(hrecv[0], from_l) + dot(hrecv[1], from_r))
    wing = jnp.concatenate(wings, axis=0)
    wing_lane = iota((group, LANES), 1)
    inside = ((wing_lane < 32) & (t > 0)) | ((wing_lane >= 32) & (wing_lane < 64) & (t < nt - 1))

    for k in range(nrow):
        zk = (rb * c + 2 * nz - 1 + k) % nz

        @pl.when(zk != z)
        def _():
            remote(tbuf.at[k], tbuf.at[k], a2s.at[0], a2r.at[k], y * nz + zk, c).wait_recv()
    blocks = [tbuf[k].astype(F32) for k in range(nrow)]
    chosen = dot(shard_n, jnp.concatenate(blocks, axis=0).astype(BF))
    for b in range(nb):
        low = (chosen[:, b * LANES:(b + 1) * LANES] * weigh).astype(BF)
        lowt = dot(fold, low, ((1,), (1,))).astype(BF)
        placed[:, b * LANES:(b + 1) * LANES] = jnp.concatenate([lowt] * (group // NBR), axis=0) * maskc[...]
    model = dot(placed[...], shifted[...])
    centre = (data[...].astype(F32) - model[:, :LANES]).astype(BF)
    res_h[...] = centre
    res[:, 0:LANES] = centre
    res[:, LANES:span] = jnp.where(inside, wing - model[:, LANES:], 0.0).astype(BF)

    own_shift = jnp.concatenate([shifted[b * LANES:b * LANES + slots, :] for b in range(nb)], axis=0)
    along = dot(own_shift, res[...], ((1,), (1,)))
    own_all = jnp.concatenate([own_mask] * nb, axis=0)
    hit = along * own_all
    feat = hit[:, 0:LANES]
    for k in range(1, group // LANES):
        feat = feat + hit[:, k * LANES:(k + 1) * LANES]
    feat = dot(feat.astype(BF), spin)
    spread_w = jnp.concatenate([feat[b * slots:(b + 1) * slots, :] * sub_own for b in range(nb)], axis=1)
    sums = dot(n_shard[:, 0:slots].astype(BF), spread_w.astype(BF))
    for k in range(nrow):
        lo, hi = k * nc, (k + 1) * nc
        ubuf[k] = jnp.concatenate([sums[lo:hi, :], tally[lo:hi, :]], axis=1).astype(BF)

    def z_of(k):
        return (rb * c + 2 * nz - 1 + k) % nz

    def to_relay(f):
        for k in range(nrow):
            dist = (z - z_of(k) + nz) % nz

            @pl.when(jnp.logical_and(dist > hop, dist <= 2 * hop))
            def _():
                at = y * nz + (z_of(k) + hop) % nz
                f(remote(ubuf.at[k], rbuf.at[dist - hop - 1], c1s.at[k], c1q.at[dist - hop - 1], at, c))

            @pl.when(jnp.logical_and(dist > 2 * hop, dist < 3 * hop))
            def _():
                at = y * nz + (z_of(k) + nz - hop) % nz
                i = 4 * hop - 1 - dist
                f(remote(ubuf.at[k], rbuf.at[i], c1s.at[k], c1q.at[i], at, c))

    def near_slot(dist):
        return jnp.where(dist <= hop, dist - 1, dist - 2 * hop)

    def to_gatherer(f):
        for k in range(nrow):
            dist = (z - z_of(k) + nz) % nz

            @pl.when(jnp.logical_or(jnp.logical_and(dist >= 1, dist < hop), dist > 3 * hop))
            def _():
                i = near_slot(dist)
                f(remote(ubuf.at[k], cbuf.at[i], c1s.at[k], c1r.at[i], y * nz + z_of(k), c))

    relays = ((hop, 0, hop), (3 * hop, hop, 2 * hop - 1))

    def relay_copy(dist):
        zt = (z - dist + nz) % nz
        k = (zt + 2 * nz - (rb * c - 1) % nz) % nz
        i = hop - 1 if dist == hop else hop
        return k, remote(ubuf.at[k], cbuf.at[i], c1s.at[k], c1r.at[i], y * nz + zt, c)

    to_relay(lambda cp: cp.start())
    to_gatherer(lambda cp: cp.start())
    for dist, lo, hi in relays:
        k, out = relay_copy(dist)

        @pl.when(k < nrow)
        def _():
            for j in range(lo, hi):
                remote(ubuf.at[0], rbuf.at[j], c1s.at[0], c1q.at[j], y * nz + (z + 1) % nz, c).wait_recv()
            part = ubuf[k].astype(F32)
            for j in range(lo, hi):
                part = part + rbuf[j].astype(F32)
            ubuf[k] = part.astype(BF)
            out.start()

    to_edge = jnp.logical_or(rr == 0, rr == nrow - 1)
    slot_out = jnp.where(to_edge, ny, 0) + y

    def c2_copy(ch):
        return remote(block8(csrc, ch), block8(dbuf, slot_out), c2s.at[ch], c2r.at[slot_out], src_row, ch)

    @pl.when(jnp.logical_not(edge))
    def _():
        dbuf[8 * ny:16 * ny, :] = jnp.zeros((8 * ny, LANES), F32)

    @pl.when(gathers)
    def _():
        for i in [j for j in range(2 * hop) if j not in (hop - 1, hop)] + [hop - 1, hop]:
            remote(ubuf.at[0], cbuf.at[i], c1s.at[0], c1r.at[i], y * nz + (z + 1) % nz, c).wait_recv()
        total = ubuf[rr].astype(F32)
        for k in range(2 * hop):
            total = total + cbuf[k].astype(F32)
        for b in range(nb + 1):
            csrc[pl.ds(b, nc, stride=8), :] = total[:, b * LANES:(b + 1) * LANES]
        csrc[pl.ds(nb + 1, nc, stride=8), :] = jnp.zeros((nc, LANES), F32)
        for ch in range(nc):
            is_own = jnp.logical_and(src_row == t, ch == c)

            @pl.when(jnp.logical_not(is_own))
            def _():
                c2_copy(ch).start()

            @pl.when(is_own)
            def _():
                block8(dbuf, slot_out)[...] = csrc[8 * ch:8 * ch + 8, :]

    for yy in range(ny):
        @pl.when(jnp.logical_or(yy != y, band != c))
        def _():
            remote(block8(csrc, 0), block8(dbuf, yy), c2s.at[0], c2r.at[yy], yy * nz + z, band).wait_recv()

        @pl.when(jnp.logical_and(edge, jnp.logical_or(yy != y, edge_band != c)))
        def _():
            remote(
                block8(csrc, 0), block8(dbuf, ny + yy), c2s.at[0], c2r.at[ny + yy], yy * nz + z, edge_band
            ).wait_recv()
    got = dbuf[0:8, :]
    for k in range(1, 2 * ny):
        got = got + dbuf[8 * k:8 * k + 8, :]
    tail = got[nb:nb + 1, :]
    number = jnp.zeros((1, LANES), F32)
    weight = jnp.zeros((1, LANES), F32)
    for u in range(PER):
        here = lane_u[0:1] == u
        number = number + jnp.where(here, tail[:, u:u + 1], 0.0)
        weight = weight + jnp.where(here, tail[:, PER + u:PER + u + 1] + tail[:, 2 * PER + u:2 * PER + u + 1], 0.0)
    fresh = (prior_weight * tblk + got + weight * gram_t) / (prior_weight + number)
    split = jnp.concatenate([jnp.where(lane_u == u, fresh, 0.0) for u in range(PER)], axis=0)
    back = joined(dot(parts(split), turn, ((1,), (1,))))
    for u in range(PER):
        piece = jnp.where(q_of == b_of, back[8 * u:8 * u + 8, :], 0.0)
        new_out[u:u + 1, :] = jnp.sum(piece, axis=0, keepdims=True)

    for yy in range(ny):
        @pl.when(jnp.logical_or(yy != y, band != c))
        def _():
            a1_copy(yy, 0).wait_send()

        @pl.when(jnp.logical_and(edge, jnp.logical_or(yy != y, edge_band != c)))
        def _():
            a1_copy(yy, 1).wait_send()
    m_right.wait_send()
    m_left.wait_send()
    h_right.wait_send()
    h_left.wait_send()

    @pl.when(gathers)
    def _():
        for d in range(1, nz):
            remote(tbuf.at[rr], tbuf.at[rr], a2s.at[d], a2r.at[rr], y * nz + (z + d) % nz, c).wait_send()
        for ch in range(nc):
            @pl.when(jnp.logical_or(src_row != t, ch != c))
            def _():
                c2_copy(ch).wait_send()
    to_relay(lambda cp: cp.wait_send())
    to_gatherer(lambda cp: cp.wait_send())
    for dist, lo, hi in relays:
        k, out = relay_copy(dist)

        @pl.when(k < nrow)
        def _():
            out.wait_send()


def shards_fn(nt, nz, nc, data, basis, templates, spike_offset, spike_unit, spike_amp, seg_count, neighbors):
    group, seg = data.shape
    nb, taps = basis.shape
    slots = spike_offset.shape[0]
    ny = nt // nz
    rb = nt // nc
    nrow = rb + 2
    row_units = nc * PER
    width = nb * LANES
    dma = pltpu.SemaphoreType.DMA
    vmem = pl.BlockSpec(memory_space=pltpu.VMEM)
    hbm = pl.BlockSpec(memory_space=pl.ANY)
    hop = nz // 4
    return pl.pallas_call(
        functools.partial(kernel, nt, nz, nc, group, taps),
        out_shape=(
            pltpu.VMEM(data.shape, BF),
            pltpu.VMEM(templates.shape, F32),
        ),
        in_specs=[hbm] * 8,
        out_specs=(vmem, vmem),
        scratch_shapes=[
            pltpu.VMEM(data.shape, BF),
            pltpu.VMEM(basis.shape, F32),
            pltpu.VMEM(templates.shape, F32),
            pltpu.VMEM((1, slots), I32),
            pltpu.VMEM((1, slots), I32),
            pltpu.VMEM((1, slots), F32),
            pltpu.VMEM((1, 1), I32),
            pltpu.VMEM((8, neighbors.shape[0]), I32),
            pltpu.VMEM(data.shape, BF),
            pltpu.VMEM((8, 2 * LANES), F32),
            pltpu.VMEM((8, LANES), F32),
            pltpu.VMEM((2, 8, LANES), F32),
            pltpu.VMEM((2, 8, LANES), F32),
            pltpu.VMEM((2, group // 4, LANES), BF),
            pltpu.VMEM((2, group // 4, LANES), BF),
            pltpu.VMEM((8, LANES), F32),
            pltpu.VMEM((8 * nc, LANES), F32),
            pltpu.VMEM((nb, 2 * LANES, 2 * LANES), BF),
            pltpu.VMEM((width, 2 * LANES), BF),
            pltpu.VMEM((group, LANES), BF),
            pltpu.VMEM((group, width), BF),
            pltpu.VMEM((group, 2 * LANES), BF),
            pltpu.VMEM((nrow, nc, width), BF),
            pltpu.VMEM((nrow, nc, width + LANES), BF),
            pltpu.VMEM((2 * hop - 1, nc, width + LANES), BF),
            pltpu.VMEM((2 * hop, nc, width + LANES), BF),
            pltpu.VMEM((8 * nc, LANES), F32),
            pltpu.VMEM((16 * ny, LANES), F32),
            dma((9,)), pltpu.SemaphoreType.REGULAR,
            dma((2,)), dma((2,)), dma((2,)), dma((2,)),
            dma((2 * ny,)), dma((nc,)),
            dma((nz,)), dma((nrow,)),
            dma((nrow,)), dma((2 * hop,)), dma((2 * hop - 1,)),
            dma((nc,)), dma((2 * ny,)),
        ],
        compiler_params=pltpu.CompilerParams(collective_id=0, has_side_effects=True),
        name="step",
    )(
        data, basis, templates,
        spike_offset.reshape(1, slots), spike_unit.reshape(1, slots), spike_amp.reshape(1, slots),
        seg_count.reshape(1, 1), neighbors.T,
    )


def solution(mesh, nz=16):
    nt, nc = mesh.shape["tm"], mesh.shape["chan"]
    return jax.shard_map(
        functools.partial(shards_fn, nt, nz, nc),
        mesh=mesh,
        in_specs=(
            P("chan", "tm"),
            P(),
            P(("tm", "chan"), None),
            P("tm"),
            P("tm"),
            P("tm"),
            P("tm"),
            P(),
        ),
        out_specs=(P("chan", "tm"), P(("tm", "chan"), None)),
        check_vma=False,
    )
```

```python
import functools

import jax
import jax.numpy as jnp
from jax import lax
from jax.experimental import pallas as pl
from jax.experimental.pallas import tpu as pltpu
from jax.sharding import PartitionSpec as P

MESH = pl.DeviceIdType.MESH
HI = lax.Precision.HIGHEST
BF = jnp.bfloat16
F32 = jnp.float32
I32 = jnp.int32
prior_weight = 4.0
LANES = 128
PER = 4
NBR = 32


def iota(shape, dim):
    return lax.broadcasted_iota(I32, shape, dim)


def dot(a, b, dims=((1,), (0,)), precision=None):
    return lax.dot_general(a, b, (dims, ((), ())), precision=precision, preferred_element_type=F32)


def one(mask, dtype=F32):
    return jnp.where(mask, 1.0, 0.0).astype(dtype)


def kernel(
    nt, nz, nc, group, taps,
    data_h, basis_h, templ_h, off_h, unit_h, amp_h, count_h, nbr_h,
    res_h, new_out,
    data, basis, templ, off, unit, amp, count, nbv, bp, mrow, msend, mrecv, hsend, hrecv, asrc, abuf, toep, shifted, maskc, placed, res,
    tbuf, uf, ef, xsrc, esrc, mbuf, ebuf, zf, zsrc, zbuf,
    nsem, vouch, msem_s, msem_r, hsem_s, hsem_r, a1s, a1r, a2s, a2r, xms, xmr, xes, xer, zss, zrs,
):
    ny = nt // nz
    rb = nt // nc
    nrow = rb + 2
    row_units = nc * PER
    nb = basis_h.shape[0]
    half = (taps - 1) // 2
    hop = nz // 4
    quarter = group // 4
    shards = nrow * nc
    width = nb * LANES
    t = lax.axis_index("tm")
    c = lax.axis_index("chan")
    y = t // nz
    z = t % nz
    band = t // rb
    at_low = (t % rb) == 0
    at_high = (t % rb) == rb - 1
    edge = jnp.logical_or(at_low, at_high)
    edge_band = jnp.where(at_low, (band + nc - 1) % nc, (band + 1) % nc)
    rr = (z + 2 * nz - (rb * c - 1) % nz) % nz
    gathers = rr < nrow
    src_row = (rb * c + nt - 1 + rr) % nt
    right = (t + 1) % nt
    left = (t + nt - 1) % nt

    barrier = pltpu.get_barrier_semaphore()

    def greet(tm, chan):
        pl.semaphore_signal(barrier, inc=1, device_id=(tm, chan), device_id_type=MESH)

    for d in range(1, hop + 1):
        greet(y * nz + (z + d) % nz, c)
        greet(y * nz + (z + nz - d) % nz, c)
    greet(right, c)
    greet(left, c)
    home = c // 2
    odd = c % 2
    beyond = jnp.where(odd == 0, (home + ny - 1) % ny, (home + 1) % ny)
    feeders = (2 * y, 2 * y + 1, (2 * y + 2) % nc, (2 * y + nc - 1) % nc)
    for ch in range(nc):
        for yo in (home, beyond):
            @pl.when(jnp.logical_or(yo != y, ch != c))
            def _():
                greet(yo * nz + z, ch)
    for yy in range(ny):
        for src in feeders:
            @pl.when(jnp.logical_or(yy != y, src != c))
            def _():
                greet(yy * nz + z, src)
    own_home = y == home
    own_beyond = y == beyond
    n_greet = 2 * hop + 2 + 2 * nc + 4 * ny
    n_greet = n_greet - jnp.where(own_home, 2, 0) - jnp.where(own_beyond, 2, 0)
    own_main = band == c
    own_edge = jnp.logical_and(edge, edge_band == c)

    def fetch(src, dst, i):
        return pltpu.make_async_copy(src, dst, nsem.at[i])

    small = [
        fetch(nbr_h.at[pl.ds(0, 8), :], nbv, 0),
        fetch(templ_h, templ, 1),
        fetch(off_h, off, 2),
        fetch(unit_h, unit, 3),
        fetch(amp_h, amp, 4),
        fetch(count_h, count, 5),
    ]
    for cp in small:
        cp.start()
    bp[...] = jnp.zeros_like(bp)
    get_data = fetch(data_h, data, 6)
    get_basis = fetch(basis_h, basis, 7)
    get_data.start()
    get_basis.start()
    mrow[...] = jnp.zeros_like(mrow)

    def parts(v):
        p0 = v.astype(BF)
        p1 = (v - p0.astype(F32)).astype(BF)
        p2 = (v - p0.astype(F32) - p1.astype(F32)).astype(BF)
        return jnp.concatenate([p0.astype(F32), p1.astype(F32), p2.astype(F32)], axis=0).astype(BF)

    def joined(v):
        n = v.shape[0] // 3
        return v[:n] + v[n:2 * n] + v[2 * n:]

    for cp in small:
        cp.wait()
    lane8 = iota((8, LANES), 1)
    row8 = iota((8, LANES), 0)
    lane_u = lane8 // NBR
    first = PER * (nc * t + c)
    mine = nbv[:, pl.ds(pl.multiple_of((first // LANES) * LANES, LANES), LANES)]
    mine = pltpu.roll(mine, (LANES - first % LANES) % LANES, 1)
    s_lane = jnp.zeros((1, LANES), I32)
    for u in range(PER):
        s_lane = s_lane + jnp.where(lane_u[0:1] == u, mine[0:1, u:u + 1], 0)
    coef = nb * NBR
    turn = one(((iota((coef, LANES), 0) + s_lane - iota((coef, LANES), 1)) & (NBR - 1)) == 0, BF)
    q_of = iota((8, coef), 1) // NBR
    b_of = iota((8, coef), 0)
    spread = jnp.concatenate([jnp.where(q_of == b_of, templ[u:u + 1, :], 0.0) for u in range(PER)], axis=0)
    turned = joined(dot(parts(spread), turn))
    tblk = jnp.zeros((8, LANES), F32)
    for u in range(PER):
        tblk = tblk + jnp.where(lane_u == u, turned[8 * u:8 * u + 8, :], 0.0)
    asrc[...] = tblk

    slots = off.shape[1]
    live = (iota((1, slots), 1) < count[...]).astype(F32)
    mrow[0:1, 0:slots] = unit[...].astype(F32)
    mrow[1:2, 0:slots] = off[...].astype(F32)
    mrow[2:3, 0:slots] = jnp.where(live > 0.0, amp[...], 0.0)
    mrow[3:4, 0:slots] = live
    meta = mrow[...]
    go_right = jnp.where(t == nt - 1, 0.0, 1.0)
    go_left = jnp.where(t == 0, 0.0, 1.0)
    seg = data_h.shape[1]
    to_right = jnp.where(row8 == 1, meta - float(seg), jnp.where(row8 >= 2, meta * go_right, meta))
    to_left = jnp.where(row8 == 1, meta + float(seg), jnp.where(row8 >= 2, meta * go_left, meta))
    to_right = jnp.where(lane8 < slots, to_right, 0.0)
    to_left = jnp.where(lane8 < slots, to_left, 0.0)
    msend[0] = pltpu.roll(to_right, slots, 1)
    msend[1] = pltpu.roll(to_left, 2 * slots, 1)

    pl.semaphore_wait(barrier, n_greet)
    for d in (hop, nz - hop):
        pl.semaphore_signal(vouch, inc=1, device_id=(y * nz + (z + d) % nz, c), device_id_type=MESH)

    def remote(src, dst, s, r, tm, chan):
        return pltpu.make_async_remote_copy(
            src_ref=src, dst_ref=dst, send_sem=s, recv_sem=r, device_id=(tm, chan), device_id_type=MESH
        )

    def block8(ref, i):
        return ref.at[pl.ds(pl.multiple_of(8 * i, 8), 8), :]

    def a1_copy(yy, e):
        return remote(asrc, block8(abuf, c), a1s.at[e * ny + yy], a1r.at[c], yy * nz + z, edge_band if e else band)

    for yy in range(ny):
        @pl.when(jnp.logical_or(yy != y, band != c))
        def _():
            a1_copy(yy, 0).start()

        @pl.when(jnp.logical_and(edge, jnp.logical_or(yy != y, edge_band != c)))
        def _():
            a1_copy(yy, 1).start()

    @pl.when(jnp.logical_or(own_main, own_edge))
    def _():
        block8(abuf, c)[...] = asrc[...]

    m_right = remote(msend.at[0], mrecv.at[0], msem_s.at[0], msem_r.at[0], right, c)
    m_left = remote(msend.at[1], mrecv.at[1], msem_s.at[1], msem_r.at[1], left, c)
    h_right = remote(hsend.at[0], hrecv.at[0], hsem_s.at[0], hsem_r.at[0], right, c)
    h_left = remote(hsend.at[1], hrecv.at[1], hsem_s.at[1], hsem_r.at[1], left, c)
    m_right.start()
    m_left.start()

    get_data.wait()
    sel_i = iota((seg, 2 * LANES), 0)
    sel_j = iota((seg, 2 * LANES), 1)
    pack = jnp.zeros((quarter, 2 * LANES), F32)
    for k in range(4):
        to_r = (sel_j == sel_i - (seg - 32) + 32 * k) & (sel_i >= seg - 32)
        to_l = (sel_j == sel_i + 32 * k + LANES) & (sel_i < 32)
        pack = pack + dot(data[k * quarter:(k + 1) * quarter, :], one(to_r | to_l, BF))
    hsend[0] = pack[:, :LANES].astype(BF)
    hsend[1] = pack[:, LANES:].astype(BF)

    h_right.start()
    h_left.start()

    get_basis.wait()
    bp[0:nb, 0:taps] = basis[...]
    span = 2 * LANES
    base = 66
    lane_s = iota((LANES, LANES), 1)

    def shifts(b):
        row = jnp.broadcast_to(bp[b:b + 1, :].astype(BF).astype(F32), (LANES, span))
        for r0 in (0, LANES):
            mid = pltpu.roll(row, (span - half - base + r0) % span, 1, stride=1, stride_axis=0)[:, :LANES]
            low = pltpu.roll(row, (span - half - base + 32 + r0) % span, 1, stride=1, stride_axis=0)[:, :LANES]
            high = pltpu.roll(row, (span - half - base - seg + 32 + r0) % span, 1, stride=1, stride_axis=0)[:, :LANES]
            side = jnp.where(lane_s < 32, low, jnp.where(lane_s < 64, high, 0.0))
            toep[b, r0:r0 + LANES, 0:LANES] = mid.astype(BF)
            toep[b, r0:r0 + LANES, LANES:span] = side.astype(BF)

    for b in range(nb):
        shifts(b)
    gram = dot(bp[...], bp[...], ((1,), (1,)), precision=HI)
    gram_t = dot(gram, tblk, precision=HI)

    pl.semaphore_wait(vouch, 2)

    @pl.when(gathers)
    def _():
        for ch in range(nc):
            @pl.when(jnp.logical_or(src_row != t, ch != c))
            def _():
                remote(asrc, block8(abuf, ch), a1s.at[0], a1r.at[ch], src_row, ch).wait_recv()
        rows = [abuf[pl.ds(b, nc, stride=8), :] for b in range(nb)]
        tbuf[rr] = jnp.concatenate(rows, axis=1).astype(BF)
        for d in [nz // 2] + [s * k for k in range(nz // 2 - 1, 0, -1) for s in (1, -1)]:
            remote(tbuf.at[rr], tbuf.at[rr], a2s.at[d % nz], a2r.at[rr], y * nz + (z + d + nz) % nz, c).start()

    m_right.wait_recv()
    m_left.wait_recv()
    every = meta + mrecv[0] + mrecv[1]
    unit_lane = every[0:1, :].astype(I32)
    shard_lane = unit_lane // PER - nc * (rb * c - 1)
    live_lane = every[3:4, :]
    stack = jnp.where(row8 == 1, every + float(base), jnp.where(row8 < 4, every, 0.0))
    cols = jnp.transpose(stack)
    unit_col = cols[:, 0:1].astype(I32)
    pos_col = cols[:, 1:2].astype(I32)
    amp_col = cols[:, 2:3]
    shard_col = unit_col // PER - nc * (rb * c - 1)
    sub_col = unit_col % PER
    n_tiles = nbv.shape[1] // LANES
    band_tiles = max(rb * row_units // LANES, 1)
    sum_start = jnp.zeros((LANES, LANES), I32)
    for k in range(min(band_tiles + 2, n_tiles)):
        tile = (c * rb * row_units // LANES - 1 + k + n_tiles) % n_tiles
        starts = nbv[:, pl.ds(pl.multiple_of(tile * LANES, LANES), LANES)][0:1]
        sum_start = sum_start + jnp.where(unit_col - tile * LANES == iota((LANES, LANES), 1), starts, 0)
    start_all = jnp.sum(sum_start.astype(F32), axis=1, keepdims=True) - float(group) * c.astype(F32)
    start_lane = jnp.transpose(jnp.broadcast_to(start_all, (LANES, LANES)))[0:1, :].astype(I32)
    start_col = start_all[0:slots].astype(I32)

    at_pos = one(pos_col == iota((LANES, span), 1), BF)
    for b in range(nb):
        shifted[b * LANES:(b + 1) * LANES, :] = dot(at_pos, toep[b]).astype(BF)
    maskc[...] = one(
        (iota((group, LANES), 0) >= start_lane) & (iota((group, LANES), 0) < start_lane + NBR), BF
    )
    own_mask = one((iota((slots, group), 1) >= start_col) & (iota((slots, group), 1) < start_col + NBR))
    shard_n = one(shard_col == iota((LANES, shards), 1), BF)
    n_shard = one(shard_lane == iota((shards, LANES), 0)) * live_lane
    lane_sub = iota((LANES, LANES), 1) // NBR
    weigh = jnp.where(lane_sub == sub_col, amp_col, 0.0)
    fold = one((iota((NBR, LANES), 1) & (NBR - 1)) == iota((NBR, LANES), 0), BF)
    spin = one((iota((LANES, LANES), 1) & (NBR - 1)) == (iota((LANES, LANES), 0) & (NBR - 1)), BF)
    sub_own = one(lane_sub == sub_col)[0:slots, :]

    l_i = iota((LANES, LANES), 1)
    kind = (l_i & 15) // PER
    match = ((l_i & (PER - 1)) == sub_col) & ((shard_col // nc) - 1 == l_i // 16) & (shard_col >= nc)
    match = match & (iota((LANES, LANES), 0) < slots)
    tally_w = jnp.where(match, jnp.where(kind == 0, 1.0, jnp.where(kind < 3, amp_col, 0.0)), 0.0)
    n_owner = one((shard_lane & (nc - 1)) == iota((8, LANES), 0)) * live_lane
    kind8 = (lane8 & 15) // PER

    def halves(v):
        coarse = v.astype(BF).astype(F32)
        return jnp.where(kind8 == 2, v - coarse, coarse)

    tally = halves(dot(n_owner, tally_w, precision=HI))

    h_right.wait_recv()
    h_left.wait_recv()
    un_i = iota((LANES, LANES), 0)
    un_j = iota((LANES, LANES), 1)
    wings = []
    for k in range(4):
        from_l = one((un_i == un_j + 32 * k) & (un_j < 32), BF)
        from_r = one((un_i == un_j - 32 + 32 * k) & (un_j >= 32) & (un_j < 64), BF)
        wings.append(dot(hrecv[0], from_l) + dot(hrecv[1], from_r))
    wing = jnp.concatenate(wings, axis=0)
    wing_lane = iota((group, LANES), 1)
    inside = ((wing_lane < 32) & (t > 0)) | ((wing_lane >= 32) & (wing_lane < 64) & (t < nt - 1))

    for k in range(nrow):
        zk = (rb * c + 2 * nz - 1 + k) % nz

        @pl.when(zk != z)
        def _():
            remote(tbuf.at[k], tbuf.at[k], a2s.at[0], a2r.at[k], y * nz + zk, c).wait_recv()
    blocks = [tbuf[k].astype(F32) for k in range(nrow)]
    chosen = dot(shard_n, jnp.concatenate(blocks, axis=0).astype(BF))
    for b in range(nb):
        low = (chosen[:, b * LANES:(b + 1) * LANES] * weigh).astype(BF)
        lowt = dot(fold, low, ((1,), (1,))).astype(BF)
        placed[:, b * LANES:(b + 1) * LANES] = jnp.concatenate([lowt] * (group // NBR), axis=0) * maskc[...]
    model = dot(placed[...], shifted[...])
    centre = (data[...].astype(F32) - model[:, :LANES]).astype(BF)
    res_h[...] = centre
    res[:, 0:LANES] = centre
    res[:, LANES:span] = jnp.where(inside, wing - model[:, LANES:], 0.0).astype(BF)

    own_shift = jnp.concatenate([shifted[b * LANES:b * LANES + slots, :] for b in range(nb)], axis=0)
    along = dot(own_shift, res[...], ((1,), (1,)))
    own_all = jnp.concatenate([own_mask] * nb, axis=0)
    hit = along * own_all
    feat = hit[:, 0:LANES]
    for k in range(1, group // LANES):
        feat = feat + hit[:, k * LANES:(k + 1) * LANES]
    feat = dot(feat.astype(BF), spin)
    spread_w = jnp.concatenate([feat[b * slots:(b + 1) * slots, :] * sub_own for b in range(nb)], axis=1)
    sums = dot(n_shard[:, 0:slots].astype(BF), spread_w.astype(BF))
    for b in range(nb):
        uf[b] = sums[:, b * LANES:(b + 1) * LANES]
    first_row, last_row = sums[:nc, :], sums[(nrow - 1) * nc:, :]
    inner = jnp.where(odd == 0, last_row, first_row)
    outer = jnp.where(odd == 0, first_row, last_row)
    blank = jnp.zeros((nc, LANES), F32)
    for b in range(nb):
        ef[0, pl.ds(b, nc, stride=8), :] = inner[:, b * LANES:(b + 1) * LANES]
        ef[1, pl.ds(b, nc, stride=8), :] = outer[:, b * LANES:(b + 1) * LANES]
    ef[0, pl.ds(nb, nc, stride=8), :] = tally[:nc]
    ef[1, pl.ds(nb, nc, stride=8), :] = blank
    for e in range(2):
        ef[e, pl.ds(nb + 1, nc, stride=8), :] = blank

    def to_home(ch):
        return remote(xsrc.at[ch], mbuf.at[odd, y], xms.at[ch], xmr.at[odd, y], home * nz + z, ch)

    def to_beyond(ch):
        return remote(esrc.at[ch], ebuf.at[odd, y], xes.at[ch], xer.at[odd, y], beyond * nz + z, ch)

    def to_owners(f):
        for ch in range(nc):
            @pl.when(jnp.logical_or(y != home, ch != c))
            def _():
                f(to_home(ch))
        for ch in range(nc):
            @pl.when(jnp.logical_or(y != beyond, ch != c))
            def _():
                f(to_beyond(ch))

    for ch in range(nc):
        pieces = [uf[b, pl.ds(nc + ch, rb, stride=nc), :] for b in range(nb)] + [ef[0, 8 * ch:8 * ch + 8, :]]
        xsrc[ch] = jnp.concatenate(pieces, axis=0).astype(BF)
        esrc[ch] = ef[1, 8 * ch:8 * ch + 8, :].astype(BF)
    to_owners(lambda cp: cp.start())

    @pl.when(own_home)
    def _():
        mbuf[odd, y] = xsrc[c]

    @pl.when(own_beyond)
    def _():
        ebuf[odd, y] = esrc[c]

    for o in range(2):
        for yy in range(ny):
            cm = 2 * y + o
            ce = feeders[2 + o]

            @pl.when(jnp.logical_or(yy != y, cm != c))
            def _():
                remote(xsrc.at[0], mbuf.at[o, yy], xms.at[0], xmr.at[o, yy], yy * nz + z, cm).wait_recv()

            @pl.when(jnp.logical_or(yy != y, ce != c))
            def _():
                remote(esrc.at[0], ebuf.at[o, yy], xes.at[0], xer.at[o, yy], yy * nz + z, ce).wait_recv()
    rest = []
    for o in range(2):
        part = mbuf[o, 0].astype(F32)
        side = ebuf[o, 0].astype(F32)
        for yy in range(1, ny):
            part = part + mbuf[o, yy].astype(F32)
            side = side + ebuf[o, yy].astype(F32)
        for b in range(nb):
            zf[pl.ds(8 * rb * o + b, rb, stride=8), :] = part[b * rb:(b + 1) * rb, :]
        tile = part[nb * rb:, :]
        merged = jnp.where(kind8 == 1, tile + pltpu.roll(tile, LANES - PER, 1), tile)
        merged = jnp.where(kind8 == 2, pltpu.roll(merged, PER, 1), merged)
        count_row = halves(merged)[nb:nb + 1, :]
        zf[pl.ds(8 * rb * o + nb, rb, stride=8), :] = jnp.broadcast_to(count_row, (rb, LANES))
        zf[pl.ds(8 * rb * o + nb + 1, rb, stride=8), :] = jnp.zeros((rb, LANES), F32)
        rest.append((jnp.where(row8 < nb, tile, 0.0), side))
    extra = {rb: rest[0][0], rb - 1: rest[1][0], nz - 1: rest[0][1], 0: rest[1][1]}
    for k in range(nz):
        tile = zf[8 * k:8 * k + 8, :]
        if k in extra:
            tile = tile + extra[k]
        zsrc[k] = tile.astype(BF)
    around = [nz // 2] + [s * k for k in range(nz // 2 - 1, 0, -1) for s in (1, -1)]

    def to_planes(f):
        for d in around:
            zt = (z + d + nz) % nz
            f(remote(zsrc.at[zt], zbuf.at[z], zss.at[d % nz], zrs.at[z], y * nz + zt, c))

    to_planes(lambda cp: cp.start())
    zbuf[z] = zsrc[z]

    for d in range(1, nz):
        zt = (z + d) % nz
        remote(zsrc.at[0], zbuf.at[zt], zss.at[0], zrs.at[zt], y * nz + zt, c).wait_recv()
    got = zbuf[0].astype(F32)
    for k in range(1, nz):
        got = got + zbuf[k].astype(F32)
    tail = pltpu.roll(got, (LANES - 16 * (z % rb)) % LANES, 1)[nb:nb + 1, :]
    number = jnp.zeros((1, LANES), F32)
    weight = jnp.zeros((1, LANES), F32)
    for u in range(PER):
        here = lane_u[0:1] == u
        number = number + jnp.where(here, tail[:, u:u + 1], 0.0)
        weight = weight + jnp.where(here, tail[:, PER + u:PER + u + 1] + tail[:, 2 * PER + u:2 * PER + u + 1], 0.0)
    fresh = (prior_weight * tblk + got + weight * gram_t) / (prior_weight + number)
    split = jnp.concatenate([jnp.where(lane_u == u, fresh, 0.0) for u in range(PER)], axis=0)
    back = joined(dot(parts(split), turn, ((1,), (1,))))
    for u in range(PER):
        piece = jnp.where(q_of == b_of, back[8 * u:8 * u + 8, :], 0.0)
        new_out[u:u + 1, :] = jnp.sum(piece, axis=0, keepdims=True)

    for yy in range(ny):
        @pl.when(jnp.logical_or(yy != y, band != c))
        def _():
            a1_copy(yy, 0).wait_send()

        @pl.when(jnp.logical_and(edge, jnp.logical_or(yy != y, edge_band != c)))
        def _():
            a1_copy(yy, 1).wait_send()
    m_right.wait_send()
    m_left.wait_send()
    h_right.wait_send()
    h_left.wait_send()

    @pl.when(gathers)
    def _():
        for d in range(1, nz):
            remote(tbuf.at[rr], tbuf.at[rr], a2s.at[d], a2r.at[rr], y * nz + (z + d) % nz, c).wait_send()
    to_owners(lambda cp: cp.wait_send())
    to_planes(lambda cp: cp.wait_send())


def shards_fn(nt, nz, nc, data, basis, templates, spike_offset, spike_unit, spike_amp, seg_count, neighbors):
    group, seg = data.shape
    nb, taps = basis.shape
    slots = spike_offset.shape[0]
    ny = nt // nz
    rb = nt // nc
    nrow = rb + 2
    row_units = nc * PER
    width = nb * LANES
    dma = pltpu.SemaphoreType.DMA
    vmem = pl.BlockSpec(memory_space=pltpu.VMEM)
    hbm = pl.BlockSpec(memory_space=pl.ANY)
    hop = nz // 4
    return pl.pallas_call(
        functools.partial(kernel, nt, nz, nc, group, taps),
        out_shape=(
            pltpu.VMEM(data.shape, BF),
            pltpu.VMEM(templates.shape, F32),
        ),
        in_specs=[hbm] * 8,
        out_specs=(vmem, vmem),
        scratch_shapes=[
            pltpu.VMEM(data.shape, BF),
            pltpu.VMEM(basis.shape, F32),
            pltpu.VMEM(templates.shape, F32),
            pltpu.VMEM((1, slots), I32),
            pltpu.VMEM((1, slots), I32),
            pltpu.VMEM((1, slots), F32),
            pltpu.VMEM((1, 1), I32),
            pltpu.VMEM((8, neighbors.shape[0]), I32),
            pltpu.VMEM((8, 2 * LANES), F32),
            pltpu.VMEM((8, LANES), F32),
            pltpu.VMEM((2, 8, LANES), F32),
            pltpu.VMEM((2, 8, LANES), F32),
            pltpu.VMEM((2, group // 4, LANES), BF),
            pltpu.VMEM((2, group // 4, LANES), BF),
            pltpu.VMEM((8, LANES), F32),
            pltpu.VMEM((8 * nc, LANES), F32),
            pltpu.VMEM((nb, 2 * LANES, 2 * LANES), BF),
            pltpu.VMEM((width, 2 * LANES), BF),
            pltpu.VMEM((group, LANES), BF),
            pltpu.VMEM((group, width), BF),
            pltpu.VMEM((group, 2 * LANES), BF),
            pltpu.VMEM((nrow, nc, width), BF),
            pltpu.VMEM((nb, nrow * nc, LANES), F32),
            pltpu.VMEM((2, 8 * nc, LANES), F32),
            pltpu.VMEM((nc, nb * rb + 8, LANES), BF),
            pltpu.VMEM((nc, 8, LANES), BF),
            pltpu.VMEM((2, ny, nb * rb + 8, LANES), BF),
            pltpu.VMEM((2, ny, 8, LANES), BF),
            pltpu.VMEM((8 * nz, LANES), F32),
            pltpu.VMEM((nz, 8, LANES), BF),
            pltpu.VMEM((nz, 8, LANES), BF),
            dma((9,)), pltpu.SemaphoreType.REGULAR,
            dma((2,)), dma((2,)), dma((2,)), dma((2,)),
            dma((2 * ny,)), dma((nc,)),
            dma((nz,)), dma((nrow,)),
            dma((nc,)), dma((2, ny)), dma((nc,)), dma((2, ny)),
            dma((nz,)), dma((nz,)),
        ],
        compiler_params=pltpu.CompilerParams(collective_id=0, has_side_effects=True),
        name="step",
    )(
        data, basis, templates,
        spike_offset.reshape(1, slots), spike_unit.reshape(1, slots), spike_amp.reshape(1, slots),
        seg_count.reshape(1, 1), neighbors.T,
    )


def solution(mesh, nz=16):
    nt, nc = mesh.shape["tm"], mesh.shape["chan"]
    return jax.shard_map(
        functools.partial(shards_fn, nt, nz, nc),
        mesh=mesh,
        in_specs=(
            P("chan", "tm"),
            P(),
            P(("tm", "chan"), None),
            P("tm"),
            P("tm"),
            P("tm"),
            P("tm"),
            P(),
        ),
        out_specs=(P("chan", "tm"), P(("tm", "chan"), None)),
        check_vma=False,
    )
```
